32 devices in a mesh: dp: 4 (over z), expert: 8 (over y, x, core).
Axes of the slice: x: 2, y: 2, z: 4, core: 2. Of those that a mesh axis runs over, the one named last changes fastest.
Arguments:
- tokens: bfloat16 [32, 212, 1024], P(('dp', 'expert')), may hold values from -6 to 6
- expert_ids: int32 [32, 212, 1], P(('dp', 'expert')), may hold values from 0 to 7; in each aligned block of 212 rows (0 to 211, 212 to 423, ..., all dimensions but the last counted through in order) at most 36 rows name the same one
- caption_lengths: int32 [32], P(('dp', 'expert')), may hold values from 1 to 16, as said below
- layer_norm_gain: float32 [1024], replicated, may hold values from 0.5 to 1.5
- router: float32 [1024, 8], replicated, may hold values from -0.1875 to 0.1875
- w_up: bfloat16 [8, 1024, 4096], P('expert', None, 'dp'), may hold values from -0.1875 to 0.1875
- w_down: bfloat16 [8, 4096, 1024], P('expert', 'dp'), may hold values from -0.09375 to 0.09375
- logit_scale: float32 [1], replicated, may hold values from 5 to 20
- logit_bias: float32 [1], replicated, may hold values from -4 to -1.5
Outputs:
- loss: float32 [1], replicated
- grad_tokens: bfloat16 [32, 212, 1024], P(('dp', 'expert'))
- grad_up: float32 [8, 1024, 4096], P('expert', None, 'dp')
- grad_down: float32 [8, 4096, 1024], P('expert', 'dp')
- grad_router: float32 [1024, 8], replicated
- layer_gain_gradient: float32 [1024], replicated
The draws below stay inside these ranges and needn't reach their ends.
Inputs may be any that keep to these rules, and one draw needn't show every extreme that they name: `expert_ids`: among the rows of one device (aligned blocks of 212 rows, devices ordered by dp then expert) no expert is named more than 36 times, a bound that some block reaches. `caption_lengths`: some caption has all 16 tokens.
All inputs are finite; a program needn't handle non-finite values.
Results may differ from the reference program's by a relative error of at most 0.009.
Values may be sent and summed in bfloat16 or wider, within the bound.
A program may use at most 128 MiB of HBM per device.

```python
import math
import jax
import jax.numpy as jnp
import numpy as np
from jax import lax

D = 1024
FF = 4096
EXPERTS = 8
PATCH = 196
CAPLEN = 16
SEQ = 212
PAIR_DEV = 1
PAIRS = 32
CAP = 36
N_DP = 4
N_EXPERT = 8


def draw_caption_lengths(key, part):
    drawn = jax.random.randint(jax.random.fold_in(key, 17), (PAIRS,), 1, CAPLEN + 1).astype(jnp.int32)
    return drawn.at[0].set(CAPLEN)


def draw_tokens(key, part):
    groups = max(PAIRS // 8, 1)
    key_member = jax.random.fold_in(key, 101)
    key_center = jax.random.fold_in(key, 102)
    key_private = jax.random.fold_in(key, 103)
    key_noise = jax.random.fold_in(key, 104)
    member = jax.random.randint(key_member, (PAIRS,), 0, groups).astype(jnp.int32)
    member_table = (member[:, None] == jnp.arange(groups, dtype=jnp.int32)[None, :]).astype(jnp.float32)
    centers = jax.random.normal(key_center, (groups, D), jnp.float32)
    center_rows = jnp.dot(member_table, centers)
    private_part = jax.random.normal(key_private, (PAIRS, D), jnp.float32)
    shared_part = 0.6 * center_rows + 0.8 * private_part
    noise_part = jax.random.normal(key_noise, (PAIRS, SEQ, D), jnp.float32)
    result_rows = 0.6 * shared_part[:, None, :] + 0.8 * noise_part
    return jnp.clip(result_rows, -6.0, 6.0).astype(jnp.bfloat16)


def level_of(own_key, dims, pieces, least, largest):
    loudness, own = 1.0, jax.random.fold_in(own_key, 6)
    for dim, blocks in pieces:
        draws = jnp.exp(jax.random.uniform(jax.random.fold_in(own, dim), (blocks,), jnp.float32, least / len(pieces), largest / len(pieces)))
        loudness = loudness * jnp.repeat(draws, dims[dim] // blocks).reshape([-1 if axis == dim else 1 for axis in range(len(dims))])
    return loudness


def deal_out(stream_key, own, number, rows, count, top, most, lean):
    order = jax.random.permutation(stream_key, count)
    packed, ordinary = shares(count, rows * top, most, lean, True), shares(count, rows * top, most, lean, False)
    places = jnp.arange(count)

    def named(sizes, turn):
        used = int((sizes > 0).sum())
        fixed = max(1, used // 4)
        moved = fixed + (places - fixed + turn * (used - fixed)) % max(1, count - fixed)
        return jnp.zeros((count,), jnp.int32).at[order[jnp.where(places < fixed, places, moved)]].set(jnp.asarray(sizes, jnp.int32))

    sizes = jnp.where(number % 4 == 0, named(packed, number // 4), named(ordinary, number - number // 4 - 1))
    mixed = jax.random.permutation(jax.random.fold_in(own, 3), count)
    donor, receiver = mixed[0:count // 2 * 2:2], mixed[1:count // 2 * 2:2]
    slack = jnp.minimum(sizes[donor] - 1, most - sizes[receiver]) // 2
    slack = jnp.where((donor == order[0]) | (receiver == order[0]) | (sizes[receiver] == 0), 0, jnp.maximum(slack, 0))
    moved = jax.random.randint(jax.random.fold_in(own, 4), (count // 2,), 0, 1 << 20) % (slack + 1)
    sizes = sizes.at[donor].add(-moved).at[receiver].add(moved)
    members = jnp.searchsorted(jnp.cumsum(sizes), jnp.arange(rows * top), side="right").astype(jnp.int32)
    table = members.reshape(top, rows).T
    table = table[jax.random.permutation(jax.random.fold_in(own, 1), rows)]
    turn = jax.random.randint(jax.random.fold_in(own, 2), (rows, 1), 0, top)
    return jnp.take_along_axis(table, (jnp.arange(top)[None, :] + turn) % top, axis=1)


def shares(number_of, total, most, lean, full):
    weights = [(1 << 20) // math.isqrt(rank ** lean) + 1 for rank in range(1, number_of + 1)]
    largest = most if full else min(most, max(-(-total // number_of), total * weights[0] // sum(weights)))
    least = 1 if total - largest >= number_of - 1 else 0
    counts, surplus = [largest] + [least] * (number_of - 1), total - largest - least * (number_of - 1)
    while surplus > 0:
        free = [i for i in range(1, number_of) if counts[i] < largest] or [i for i in range(1, number_of) if counts[i] < most]
        mass, remaining = sum([weights[i] for i in free]), surplus
        for i in free:
            more = min(most - counts[i], max(1, remaining * weights[i] // mass), surplus)
            counts[i] = counts[i] + more
            surplus = surplus - more
    return np.array(counts)


def bell_draw(stream_key, shape, spread, reach, split=(), held_as=jnp.bfloat16):
    entries = jax.random.normal(stream_key, shape, jnp.float32) * spread
    if len(split) > 0:
        entries = level_of(stream_key, shape, split, -0.22, 0.18) * entries
    return jnp.clip(entries, min=-reach, max=reach).astype(held_as)


def setup_inputs(seed: int = 0) -> dict:
    key_of = jax.random.split(jax.random.key(seed), 10)
    tokens = draw_tokens(jax.random.fold_in(key_of[9], 71), 0)
    expert_ids_keys = jax.random.split(jax.random.fold_in(key_of[1], 1), PAIRS * SEQ // (PAIR_DEV * SEQ))
    expert_ids_turns = jax.random.permutation(jax.random.fold_in(key_of[1], 3), PAIRS * SEQ // (PAIR_DEV * SEQ))
    expert_ids = jax.vmap(lambda own, number: deal_out(jax.random.fold_in(key_of[1], 2), own, number, PAIR_DEV * SEQ, EXPERTS, 1, CAP, 2))(expert_ids_keys, expert_ids_turns).reshape((PAIRS, SEQ, 1))
    caption_lengths = draw_caption_lengths(jax.random.fold_in(key_of[9], 71), 0)
    layer_norm_gain = jnp.clip(1.0 + 0.1 * jax.random.normal(key_of[3], (D,), jnp.float32), 0.5, 1.5)
    router = bell_draw(key_of[4], (D, EXPERTS), D ** -0.5, 0.1875, (), jnp.float32)
    w_up = bell_draw(key_of[5], (EXPERTS, D, FF), D ** -0.5, 0.1875, ((0, 8), (2, 4)))
    w_down = bell_draw(key_of[6], (EXPERTS, FF, D), FF ** -0.5, 0.09375, ((0, 8), (1, 4)))
    logit_scale = jnp.clip(jnp.exp(jax.random.uniform(key_of[7], (1,), jnp.float32, math.log(5.0), math.log(20.0))), 5.0, 20.0)
    logit_bias = jnp.clip(jax.random.uniform(key_of[8], (1,), jnp.float32, -4.0, -1.5), -4.0, -1.5)
    return {"tokens": tokens, "expert_ids": expert_ids, "caption_lengths": caption_lengths, "layer_norm_gain": layer_norm_gain, "router": router, "w_up": w_up, "w_down": w_down, "logit_scale": logit_scale, "logit_bias": logit_bias}


eps = 1e-06
loss_scale = 1024.0

def gelu_slope(pre):
    return 0.5 * (1.0 + lax.erf(pre * 0.7071067811865476)) + pre * jnp.exp(-0.5 * pre * pre) * 0.3989422804014327

def group_sum(parts):
    rounded = lax.optimization_barrier(parts.astype(jnp.bfloat16))
    return lax.optimization_barrier(jnp.sum(rounded.astype(jnp.float32), axis=0)).astype(jnp.bfloat16)

def reference(tokens, expert_ids, caption_lengths, layer_norm_gain, router, w_up, w_down, logit_scale, logit_bias):
    devices = N_DP * N_EXPERT
    rows_dev = PAIR_DEV * SEQ
    total = PAIRS * SEQ
    ffd = FF // N_DP
    input_rows = tokens.reshape(total, D).astype(jnp.float32)
    input_mean = lax.optimization_barrier(jnp.mean(input_rows, axis=1, keepdims=True))
    var_x = lax.optimization_barrier(jnp.mean((input_rows - input_mean) ** 2, axis=1, keepdims=True))
    inverse_deviation = 1.0 / jnp.sqrt(var_x + eps)
    centered_scaled_input = (input_rows - input_mean) * inverse_deviation
    normalized_input = (centered_scaled_input * layer_norm_gain).astype(jnp.bfloat16)
    ids = expert_ids.reshape(total).astype(jnp.int32)
    onehot = (ids[:, None] == jnp.arange(EXPERTS, dtype=jnp.int32)[None, :]).astype(jnp.int32)
    blocks = onehot.reshape(devices, rows_dev, EXPERTS)
    slot = lax.optimization_barrier(jnp.sum((jnp.cumsum(blocks, axis=1) - 1) * blocks, axis=2)).reshape(total)
    owner = jnp.arange(total, dtype=jnp.int32) // rows_dev
    dest = ids * (devices * CAP) + owner * CAP + slot
    xe = jnp.zeros((EXPERTS * devices * CAP, D), jnp.bfloat16).at[dest].set(normalized_input).reshape(EXPERTS, devices * CAP, D)

    def forward_one(operands):
        rows, wu, wd = operands
        pre = jnp.dot(rows, wu, preferred_element_type=jnp.float32)
        act = jax.nn.gelu(pre, approximate=False).astype(jnp.bfloat16)
        parts = jnp.einsum('rqf,qfd->qrd', act.astype(jnp.float32).reshape(-1, N_DP, ffd), wd.astype(jnp.float32).reshape(N_DP, ffd, D))
        return group_sum(parts)
    out_e = lax.map(forward_one, (xe, w_up, w_down))
    moe = out_e.reshape(-1, D)[dest].astype(jnp.float32)
    xnf = normalized_input.astype(jnp.float32)
    router_logits = jnp.dot(xnf, router, precision=lax.Precision.HIGHEST)
    gate = jax.nn.sigmoid(lax.optimization_barrier(jnp.sum(router_logits * onehot.astype(jnp.float32), axis=1)))
    y = (input_rows + gate[:, None] * moe).reshape(PAIRS, SEQ, D)
    img = lax.optimization_barrier(jnp.mean(y[:, :PATCH], axis=1))
    lengths = caption_lengths.astype(jnp.float32)
    mask = (jnp.arange(CAPLEN, dtype=jnp.int32)[None, :] < caption_lengths[:, None]).astype(jnp.float32)
    txt = lax.optimization_barrier(jnp.sum(y[:, PATCH:] * mask[:, :, None], axis=1)) / lengths[:, None]
    ru = jnp.sqrt(lax.optimization_barrier(jnp.mean(img * img, axis=1, keepdims=True)) + eps)
    rv = jnp.sqrt(lax.optimization_barrier(jnp.mean(txt * txt, axis=1, keepdims=True)) + eps)
    u = img / ru
    v = txt / rv
    scale = logit_scale[0]
    logits = scale * jnp.dot(u, v.T, precision=lax.Precision.HIGHEST) / D + logit_bias[0]
    sign = 2.0 * jnp.eye(PAIRS, dtype=jnp.float32) - 1.0
    loss = -jnp.sum(jax.nn.log_sigmoid(sign * logits)) / PAIRS
    coef = -(loss_scale / PAIRS) * sign * jax.nn.sigmoid(-sign * logits)
    du = scale / D * jnp.dot(coef, v, precision=lax.Precision.HIGHEST)
    dv = scale / D * jnp.dot(coef.T, u, precision=lax.Precision.HIGHEST)
    dimg = (du - u * lax.optimization_barrier(jnp.mean(du * u, axis=1, keepdims=True))) / ru
    dtxt = (dv - v * lax.optimization_barrier(jnp.mean(dv * v, axis=1, keepdims=True))) / rv
    dy_img = jnp.broadcast_to(dimg[:, None, :] / PATCH, (PAIRS, PATCH, D))
    dy_txt = (dtxt / lengths[:, None])[:, None, :] * mask[:, :, None]
    dy = jnp.concatenate([dy_img, dy_txt], axis=1).reshape(total, D)
    dmoe = (gate[:, None] * dy).astype(jnp.bfloat16)
    dgl = lax.optimization_barrier(jnp.sum(dy * moe, axis=1)) * gate * (1.0 - gate)
    grad_router = jnp.dot(xnf.T, onehot.astype(jnp.float32) * dgl[:, None], precision=lax.Precision.HIGHEST)
    dme = jnp.zeros((EXPERTS * devices * CAP, D), jnp.bfloat16).at[dest].set(dmoe).reshape(EXPERTS, devices * CAP, D)

    def backward_one(operands):
        rows, grads, wu, wd = operands
        pre = jnp.dot(rows, wu, preferred_element_type=jnp.float32)
        act = jax.nn.gelu(pre, approximate=False).astype(jnp.bfloat16)
        dact = jnp.dot(grads, wd.T, preferred_element_type=jnp.float32)
        dpre = (dact * gelu_slope(pre)).astype(jnp.bfloat16)
        g_down = jnp.dot(act.T, grads, preferred_element_type=jnp.float32)
        g_up = jnp.dot(rows.T, dpre, preferred_element_type=jnp.float32)
        parts = jnp.einsum('rqf,dqf->qrd', dpre.astype(jnp.float32).reshape(-1, N_DP, ffd), wu.astype(jnp.float32).reshape(D, N_DP, ffd))
        return (g_up, g_down, group_sum(parts))
    grad_up, grad_down, dxe = lax.map(backward_one, (xe, dme, w_up, w_down))
    router_rows = jnp.dot(onehot.astype(jnp.float32), router.T, precision=lax.Precision.HIGHEST)
    gradient_normalized_input = dxe.reshape(-1, D)[dest].astype(jnp.float32) + dgl[:, None] * router_rows
    layer_gain_gradient = lax.optimization_barrier(jnp.sum(gradient_normalized_input * centered_scaled_input, axis=0))
    scaled_output_gradient = gradient_normalized_input * layer_norm_gain
    normed_input_gradient = (scaled_output_gradient - lax.optimization_barrier(jnp.mean(scaled_output_gradient, axis=1, keepdims=True)) - centered_scaled_input * lax.optimization_barrier(jnp.mean(scaled_output_gradient * centered_scaled_input, axis=1, keepdims=True))) * inverse_deviation
    grad_tokens = (dy + normed_input_gradient).astype(jnp.bfloat16).reshape(PAIRS, SEQ, D)
    return (loss.reshape(1), grad_tokens, grad_up, grad_down, grad_router, layer_gain_gradient)
```

```python
import functools

import jax
import jax.numpy as jnp
from jax import lax
from jax.experimental import pallas as pl
from jax.experimental.pallas import tpu as pltpu
from jax.sharding import PartitionSpec as P

D = 1024
PATCH = 196
CAPLEN = 16
SEQ = 212

eps = 1e-06
loss_scale = 1024.0
MESH = pl.DeviceIdType.MESH
HIGHEST = lax.Precision.HIGHEST


def gelu_slope(pre):
    return (
        0.5 * (1.0 + lax.erf(pre * 0.7071067811865476))
        + pre * jnp.exp(-0.5 * pre * pre) * 0.3989422804014327
    )


def split(value):
    high = lax.reduce_precision(value, 8, 7)
    return high.astype(jnp.bfloat16), (value - high).astype(jnp.bfloat16)


def dot(a, b, contract):
    return lax.dot_general(a, b, (contract, ((), ())), preferred_element_type=jnp.float32)


def vmem():
    return pl.BlockSpec(memory_space=pltpu.VMEM)


def dispatch_kernel(nd, ne, x_ref, out_ref, own_sem, a_sem, up_sem, dn_sem, r_sem):
    z = lax.axis_index("dp")
    e = lax.axis_index("expert")

    def hop(o, s, step, sem):
        return pltpu.make_async_remote_copy(
            src_ref=out_ref.at[o, s],
            dst_ref=out_ref.at[o, s],
            send_sem=sem.at[o, s],
            recv_sem=r_sem.at[o, s],
            device_id=(z + step, e),
            device_id_type=MESH,
        )

    def cross(t):
        return pltpu.make_async_remote_copy(
            src_ref=x_ref.at[t],
            dst_ref=out_ref.at[z, e],
            send_sem=a_sem.at[t],
            recv_sem=r_sem.at[z, e],
            device_id=(z, t),
            device_id_type=MESH,
        )

    def forward_up(o, s):
        @pl.when(z < nd - 1)
        def _():
            hop(o, s, 1, up_sem).start()

    def forward_dn(o, s):
        @pl.when(z > 0)
        def _():
            hop(o, s, -1, dn_sem).start()

    own = pltpu.make_async_copy(x_ref.at[e], out_ref.at[z, e], own_sem)
    own.start()

    @pl.loop(1, ne)
    def _(k):
        cross(lax.rem(e + k, ne)).start()

    own.wait()
    forward_up(z, e)
    forward_dn(z, e)

    @pl.loop(1, ne)
    def _(k):
        s = lax.rem(e + ne - k, ne)
        hop(z, s, 0, up_sem).wait_recv()
        forward_up(z, s)
        forward_dn(z, s)

    for d in range(1, nd):

        @pl.loop(0, ne)
        def _(k):
            s = lax.rem(e + ne - k, ne)

            @pl.when(z - d >= 0)
            def _():
                hop(z - d, s, 0, up_sem).wait_recv()
                forward_up(z - d, s)

            @pl.when(z + d < nd)
            def _():
                hop(z + d, s, 0, up_sem).wait_recv()
                forward_dn(z + d, s)

    @pl.loop(1, ne)
    def _(k):
        cross(lax.rem(e + k, ne)).wait_send()

    @pl.loop(0, nd)
    def _(o):
        @pl.loop(0, ne)
        def _(s):
            @pl.when((z < nd - 1) & (o <= z))
            def _():
                hop(o, s, 0, up_sem).wait_send()

            @pl.when((z > 0) & (o >= z))
            def _():
                hop(o, s, 0, dn_sem).wait_send()


def dispatch(buffer, nd, ne):
    _, height, width = buffer.shape
    return pl.pallas_call(
        functools.partial(dispatch_kernel, nd, ne),
        out_shape=jax.ShapeDtypeStruct((nd, ne, height, width), buffer.dtype),
        in_specs=[vmem()],
        out_specs=vmem(),
        scratch_shapes=[
            pltpu.SemaphoreType.DMA,
            pltpu.SemaphoreType.DMA((ne,)),
            pltpu.SemaphoreType.DMA((nd, ne)),
            pltpu.SemaphoreType.DMA((nd, ne)),
            pltpu.SemaphoreType.DMA((nd, ne)),
        ],
        compiler_params=pltpu.CompilerParams(has_side_effects=True),
        name="dispatch",
    )(buffer)


def bring_kernel(
    nd, ne, b_ref, ret_ref, from_dn, from_up, fin, up_sem, dn_sem, ru_sem, rd_sem, a_sem, ra_sem
):
    z = lax.axis_index("dp")
    e = lax.axis_index("expert")

    def rise(src, o, s):
        return pltpu.make_async_remote_copy(
            src_ref=src.at[o, s],
            dst_ref=from_dn.at[o, s],
            send_sem=up_sem.at[o, s],
            recv_sem=ru_sem.at[o, s],
            device_id=(z + 1, e),
            device_id_type=MESH,
        )

    def fall(src, o, s):
        return pltpu.make_async_remote_copy(
            src_ref=src.at[o, s],
            dst_ref=from_up.at[o, s],
            send_sem=dn_sem.at[o, s],
            recv_sem=rd_sem.at[o, s],
            device_id=(z - 1, e),
            device_id_type=MESH,
        )

    def cross(s):
        return pltpu.make_async_remote_copy(
            src_ref=fin.at[s],
            dst_ref=ret_ref.at[e],
            send_sem=a_sem.at[s],
            recv_sem=ra_sem.at[e],
            device_id=(z, s),
            device_id_type=MESH,
        )

    def back(s):
        return pltpu.make_async_remote_copy(
            src_ref=fin.at[s],
            dst_ref=ret_ref.at[s],
            send_sem=a_sem.at[s],
            recv_sem=ra_sem.at[s],
            device_id=(z, s),
            device_id_type=MESH,
        )

    def add(held, o, s):
        total = held[o, s].astype(jnp.float32) + b_ref[o, s].astype(jnp.float32)
        held[o, s] = total.astype(held.dtype)

    for j in range(nd - 1):
        high, low = nd - 1 - j, j

        @pl.loop(0, ne)
        def _(k):
            s = lax.rem(e + k + 1, ne)

            @pl.when((high > z) & (z == 0))
            def _():
                rise(b_ref, high, s).start()

            @pl.when((high > z) & (z > 0))
            def _():
                rise(from_dn, high, s).wait_recv()
                add(from_dn, high, s)
                rise(from_dn, high, s).start()

            @pl.when((low < z) & (z == nd - 1))
            def _():
                fall(b_ref, low, s).start()

            @pl.when((low < z) & (z < nd - 1))
            def _():
                fall(from_up, low, s).wait_recv()
                add(from_up, low, s)
                fall(from_up, low, s).start()

    @pl.loop(0, ne)
    def _(k):
        s = lax.rem(e + k + 1, ne)
        fin[s] = b_ref[z, s]

        @pl.when(z > 0)
        def _():
            rise(from_dn, z, s).wait_recv()
            fin[s] = (fin[s].astype(jnp.float32) + from_dn[z, s].astype(jnp.float32)).astype(
                fin.dtype
            )

        @pl.when(z < nd - 1)
        def _():
            fall(from_up, z, s).wait_recv()
            fin[s] = (fin[s].astype(jnp.float32) + from_up[z, s].astype(jnp.float32)).astype(
                fin.dtype
            )

        @pl.when(s != e)
        def _():
            cross(s).start()

        @pl.when(s == e)
        def _():
            ret_ref[e] = fin[e]

    @pl.loop(1, ne)
    def _(k):
        back(lax.rem(e + ne - k, ne)).wait_recv()

    @pl.loop(1, ne)
    def _(k):
        cross(lax.rem(e + k, ne)).wait_send()

    @pl.loop(0, nd)
    def _(o):
        @pl.loop(0, ne)
        def _(s):
            @pl.when(o > z)
            def _():
                rise(b_ref, o, s).wait_send()

            @pl.when(o < z)
            def _():
                fall(b_ref, o, s).wait_send()


def bring_back(partial_rows, nd, ne):
    _, _, height, width = partial_rows.shape
    dtype = partial_rows.dtype
    dma = pltpu.SemaphoreType.DMA
    return pl.pallas_call(
        functools.partial(bring_kernel, nd, ne),
        out_shape=jax.ShapeDtypeStruct((ne, height, width), dtype),
        in_specs=[vmem()],
        out_specs=vmem(),
        scratch_shapes=[
            pltpu.VMEM((nd, ne, height, width), dtype),
            pltpu.VMEM((nd, ne, height, width), dtype),
            pltpu.VMEM((ne, height, width), dtype),
            dma((nd, ne)),
            dma((nd, ne)),
            dma((nd, ne)),
            dma((nd, ne)),
            dma((ne,)),
            dma((ne,)),
        ],
        compiler_params=pltpu.CompilerParams(has_side_effects=True),
        name="bring_back",
    )(partial_rows)


def spread(nd, ne, me, src, dst, send_sem, recv_sem):
    n = nd * ne

    def copy(t, sender):
        return pltpu.make_async_remote_copy(
            src_ref=src(t),
            dst_ref=dst.at[sender],
            send_sem=send_sem.at[t],
            recv_sem=recv_sem.at[sender],
            device_id=(t // ne, lax.rem(t, ne)),
            device_id_type=MESH,
        )

    @pl.loop(1, n)
    def _(k):
        copy(lax.rem(me + k, n), me).start()

    @pl.loop(1, n)
    def _(k):
        t = lax.rem(me + n - k, n)
        copy(t, t).wait_recv()

    return copy


def drain(n, me, copy):
    @pl.loop(1, n)
    def _(k):
        copy(lax.rem(me + k, n), me).wait_send()


def pairs_kernel(nd, ne, m_ref, x_ref, out_ref, held, own, s1, r1, s2, r2):
    n = nd * ne
    me = lax.axis_index("dp") * ne + lax.axis_index("expert")
    held[me] = m_ref[me]
    first = spread(nd, ne, me, lambda t: m_ref.at[t], held, s1, r1)
    total = jnp.sum(held[...], axis=0) + x_ref[...]
    own[...] = total
    out_ref[me] = total
    second = spread(nd, ne, me, lambda t: own, out_ref, s2, r2)
    drain(n, me, first)
    drain(n, me, second)


def pair_sums(m, x, nd, ne):
    n = nd * ne
    dma = pltpu.SemaphoreType.DMA
    return pl.pallas_call(
        functools.partial(pairs_kernel, nd, ne),
        out_shape=jax.ShapeDtypeStruct(m.shape, m.dtype),
        in_specs=[vmem(), vmem()],
        out_specs=vmem(),
        scratch_shapes=[
            pltpu.VMEM(m.shape, m.dtype),
            pltpu.VMEM(x.shape, x.dtype),
            dma((n,)),
            dma((n,)),
            dma((n,)),
            dma((n,)),
        ],
        compiler_params=pltpu.CompilerParams(has_side_effects=True),
        name="pair_sums",
    )(m, x)


def everyone_kernel(nd, ne, x_ref, out_ref, s1, r1):
    n = nd * ne
    me = lax.axis_index("dp") * ne + lax.axis_index("expert")
    out_ref[me] = x_ref[...]
    drain(n, me, spread(nd, ne, me, lambda t: x_ref, out_ref, s1, r1))


def everyone(x, nd, ne):
    n = nd * ne
    dma = pltpu.SemaphoreType.DMA
    return pl.pallas_call(
        functools.partial(everyone_kernel, nd, ne),
        out_shape=jax.ShapeDtypeStruct((n,) + x.shape, x.dtype),
        in_specs=[vmem()],
        out_specs=vmem(),
        scratch_shapes=[dma((n,)), dma((n,))],
        compiler_params=pltpu.CompilerParams(has_side_effects=True),
        name="everyone",
    )(x)


def body(
    tokens,
    expert_ids,
    caption_lengths,
    layer_norm_gain,
    router,
    w_up,
    w_down,
    logit_scale,
    logit_bias,
):
    nd = lax.axis_size("dp")
    ne = lax.axis_size("expert")
    n = nd * ne
    assert tokens.shape[0] == 1 and w_up.shape[0] == 1
    rows = SEQ
    experts = router.shape[1]
    slots = rows * 4 // (3 * experts) + 1
    height = -(-(slots + 1) // 8) * 8
    total = n * height
    expert = lax.axis_index("expert")
    me = lax.axis_index("dp") * ne + expert
    wu, wd = w_up[0], w_down[0]

    x = tokens.reshape(rows, D).astype(jnp.float32)
    mean = jnp.mean(x, axis=1, keepdims=True)
    var = jnp.mean((x - mean) ** 2, axis=1, keepdims=True)
    rstd = 1.0 / jnp.sqrt(var + eps)
    xhat = (x - mean) * rstd
    xn = (xhat * layer_norm_gain).astype(jnp.bfloat16)

    ids = expert_ids.reshape(rows)
    onehot = ids[:, None] == jnp.arange(experts, dtype=jnp.int32)[None, :]
    earlier = jnp.arange(rows)[:, None] > jnp.arange(rows)[None, :]
    before = dot(earlier.astype(jnp.bfloat16), onehot.astype(jnp.bfloat16), ((1,), (0,)))
    slot = jnp.sum(jnp.where(onehot, before, 0.0), axis=1).astype(jnp.int32)
    dest = ids * height + slot
    place = (jnp.arange(experts * height, dtype=jnp.int32)[:, None] == dest[None, :]).astype(
        jnp.bfloat16
    )
    length = caption_lengths.astype(jnp.float32)
    row = jnp.arange(rows, dtype=jnp.int32)
    mark = jnp.where(row < PATCH, -1.0, jnp.where(row - PATCH < caption_lengths[0], length[0], 0.0))
    marks = jnp.sum(place.astype(jnp.float32) * mark[None, :], axis=1).reshape(experts, 1, height)
    marks = jnp.pad(marks, ((0, 0), (0, 0), (0, D - height)))
    packed = dot(place, xn, ((1,), (0,))).reshape(experts, height, D)
    is_mark = (jnp.arange(height) == slots)[None, :, None]
    packed = jnp.where(is_mark, marks, packed).astype(jnp.bfloat16)

    got = dispatch(packed, nd, ne)
    xe = got.reshape(total, D)

    marks = got.reshape(n, height, D)[:, slots, :height].astype(jnp.float32)
    marks = jnp.where(jnp.arange(height)[None, :] < slots, marks, 0.0).reshape(total)
    is_img, is_txt = marks < 0.0, marks > 0.0
    weight = jnp.where(is_img, 1.0 / PATCH, jnp.where(is_txt, 1.0 / jnp.maximum(marks, 1.0), 0.0))
    column = lax.dynamic_slice_in_dim(router, expert, 1, axis=1)[:, 0]
    xef = xe.astype(jnp.float32)
    gate = jax.nn.sigmoid(jnp.sum(xef * column[None, :], axis=1))
    coef_row = weight * gate
    pre = dot(xe, wu, ((1,), (0,)))
    act = jax.nn.gelu(pre, approximate=False).astype(jnp.bfloat16)
    kind = jnp.arange(2 * n, dtype=jnp.int32)[:, None]
    pair_of = jnp.arange(total, dtype=jnp.int32)[None, :] // height
    member = (kind // 2 == pair_of) & ((kind % 2 == 0) == is_img[None, :])
    q_high, q_low = split(jnp.where(member, coef_row[None, :], 0.0))
    both = dot(jnp.concatenate([q_high, q_low], axis=0), act, ((1,), (0,)))
    a = both[: 2 * n] + both[2 * n :]
    a_high, a_low = split(a)
    both = dot(jnp.concatenate([a_high, a_low], axis=0), wd, ((1,), (0,)))
    moe_sums = both[: 2 * n] + both[2 * n :]

    img_x = jnp.sum(x[:PATCH], axis=0) / PATCH
    mask = (jnp.arange(CAPLEN, dtype=jnp.int32) < caption_lengths[0]).astype(jnp.float32)
    txt_x = jnp.sum(x[PATCH:] * mask[:, None], axis=0) / length[0]
    own_x = jnp.concatenate([img_x, txt_x]).reshape(8, 2 * D // 8)
    sums = pair_sums(moe_sums.reshape(n, 8, 2 * D // 8), own_x, nd, ne).reshape(n, 2, D)
    img, txt = sums[:, 0], sums[:, 1]

    ru = jnp.sqrt(jnp.mean(img * img, axis=1, keepdims=True) + eps)
    rv = jnp.sqrt(jnp.mean(txt * txt, axis=1, keepdims=True) + eps)
    u, v = img / ru, txt / rv
    scale = logit_scale[0]
    logits = (
        scale * lax.dot_general(u, v, (((1,), (1,)), ((), ())), precision=HIGHEST) / D
        + logit_bias[0]
    )
    sign = 2.0 * jnp.eye(n, dtype=jnp.float32) - 1.0
    loss = -jnp.sum(jax.nn.log_sigmoid(sign * logits)) / n
    coef = -(loss_scale / n) * sign * jax.nn.sigmoid(-sign * logits)
    du = scale / D * jnp.dot(coef, v, precision=HIGHEST)
    dv = scale / D * lax.dot_general(coef, u, (((0,), (0,)), ((), ())), precision=HIGHEST)
    dimg = (du - u * jnp.mean(du * u, axis=1, keepdims=True)) / ru
    dtxt = (dv - v * jnp.mean(dv * v, axis=1, keepdims=True)) / rv
    dvec = jnp.stack([dimg, dtxt], axis=1).reshape(2 * n, D)
    d_high, d_low = split(dvec)

    both = dot(jnp.concatenate([d_high, d_low], axis=0), wd, ((1,), (1,)))
    dhid = (both[: 2 * n] + both[2 * n :]).reshape(n, 2, 1, -1)
    chosen = jnp.where(is_img.reshape(n, height, 1), dhid[:, 0], dhid[:, 1]).reshape(total, -1)
    dgl = jnp.sum(act.astype(jnp.float32) * chosen, axis=1) * weight * gate * (1.0 - gate)
    dpre = (coef_row[:, None] * chosen * gelu_slope(pre)).astype(jnp.bfloat16)
    back = (dot(dpre, wu, ((1,), (1,))) + dgl[:, None] * column[None, :]).astype(jnp.bfloat16)
    returned = bring_back(back.reshape(nd, ne, height, D), nd, ne)
    grad_up = dot(xe, dpre, ((0,), (0,)))[None]
    grad_down = dot(
        jnp.concatenate([a_high, a_high, a_low], axis=0),
        jnp.concatenate([d_high, d_low, d_high], axis=0),
        ((0,), (0,)),
    )[None]
    router_part = jnp.sum(xef * dgl[:, None], axis=0)

    dxn = dot(place, returned.reshape(experts * height, D), ((0,), (0,)))
    gain_part = jnp.sum(dxn * xhat, axis=0)
    g = dxn * layer_norm_gain
    normed = (
        g - jnp.mean(g, axis=1, keepdims=True) - xhat * jnp.mean(g * xhat, axis=1, keepdims=True)
    ) * rstd
    mine = lax.dynamic_slice_in_dim(dvec, 2 * me, 2, axis=0)
    dy = jnp.where(
        (row < PATCH)[:, None],
        mine[0:1] / PATCH,
        jnp.where(mark > 0.0, 1.0 / length[0], 0.0)[:, None] * mine[1:2],
    )
    grad_tokens = (dy + normed).astype(jnp.bfloat16).reshape(1, SEQ, D)
    last = everyone(jnp.concatenate([gain_part, router_part]).reshape(8, 2 * D // 8), nd, ne)
    last = last.reshape(nd, ne, 2, D)
    gain_grad = jnp.sum(last[:, :, 0], axis=(0, 1))
    grad_router = jnp.sum(last[:, :, 1], axis=0).T
    return (loss.reshape(1), grad_tokens, grad_up, grad_down, grad_router, gain_grad)


def solution(mesh):
    return jax.shard_map(
        body,
        mesh=mesh,
        in_specs=(
            P(("dp", "expert"), None, None),
            P(("dp", "expert"), None, None),
            P(("dp", "expert")),
            P(),
            P(),
            P("expert", None, "dp"),
            P("expert", "dp", None),
            P(),
            P(),
        ),
        out_specs=(
            P(),
            P(("dp", "expert"), None, None),
            P("expert", None, "dp"),
            P("expert", "dp", None),
            P(),
            P(),
        ),
        check_vma=False,
    )
```

```python
import functools

import jax
import jax.numpy as jnp
from jax import lax
from jax.experimental import pallas as pl
from jax.experimental.pallas import tpu as pltpu
from jax.sharding import PartitionSpec as P

D = 1024
PATCH = 196
CAPLEN = 16
SEQ = 212

eps = 1e-06
loss_scale = 1024.0
MESH = pl.DeviceIdType.MESH
HIGHEST = lax.Precision.HIGHEST


def split(value):
    high = lax.reduce_precision(value, 8, 7)
    return high.astype(jnp.bfloat16), (value - high).astype(jnp.bfloat16)


def split3(value):
    high = lax.reduce_precision(value, 8, 7)
    return (high.astype(jnp.bfloat16),) + split(value - high)


def dot(a, b, contract):
    return lax.dot_general(a, b, (contract, ((), ())), preferred_element_type=jnp.float32)


def vmem():
    return pl.BlockSpec(memory_space=pltpu.VMEM)


def dispatch_kernel(
    nd, ne, x_ref, w_ref, out_ref, act_ref, slope_ref, own_sem, a_sem, up_sem, dn_sem, r_sem
):
    _, height, width = x_ref.shape
    hidden = w_ref.shape[1]
    tiles = hidden // 128
    every = ne // tiles
    z = lax.axis_index("dp")
    e = lax.axis_index("expert")

    def hop(o, s, step, sem):
        return pltpu.make_async_remote_copy(
            src_ref=out_ref.at[o, s],
            dst_ref=out_ref.at[o, s],
            send_sem=sem.at[o, s],
            recv_sem=r_sem.at[o, s],
            device_id=(z + step, e),
            device_id_type=MESH,
        )

    def cross(t):
        return pltpu.make_async_remote_copy(
            src_ref=x_ref.at[t],
            dst_ref=out_ref.at[z, e],
            send_sem=a_sem.at[t],
            recv_sem=r_sem.at[z, e],
            device_id=(z, t),
            device_id_type=MESH,
        )

    def forward_up(o, s):
        @pl.when(z < nd - 1)
        def _():
            hop(o, s, 1, up_sem).start()

    def forward_dn(o, s):
        @pl.when(z > 0)
        def _():
            hop(o, s, -1, dn_sem).start()

    def compute(o, k):
        cols = pl.ds(pl.multiple_of(k // every * 128, 128), 128)
        xe = out_ref[o].reshape(ne * height, width)
        pre = jnp.dot(xe, w_ref[:, cols], preferred_element_type=jnp.float32)
        half = 0.5 * (1.0 + lax.erf(pre * 0.7071067811865476))
        bell = jnp.exp(-0.5 * pre * pre) * 0.3989422804014327
        act_ref[o, :, cols] = (pre * half).astype(jnp.bfloat16)
        slope_ref[o, :, cols] = half + pre * bell

    def compute_ring(d, k):
        @pl.when(lax.rem(k, every) == 0)
        def _():
            @pl.when(z - d >= 0)
            def _():
                compute(z - d, k)

            if d > 0:

                @pl.when(z + d < nd)
                def _():
                    compute(z + d, k)

    own = pltpu.make_async_copy(x_ref.at[e], out_ref.at[z, e], own_sem)
    own.start()

    @pl.loop(1, ne)
    def _(k):
        cross(lax.rem(e + k, ne)).start()

    own.wait()
    forward_up(z, e)
    forward_dn(z, e)

    @pl.loop(1, ne)
    def _(k):
        s = lax.rem(e + ne - k, ne)
        hop(z, s, 0, up_sem).wait_recv()
        forward_up(z, s)
        forward_dn(z, s)

    for d in range(1, nd):

        @pl.loop(0, ne)
        def _(k):
            s = lax.rem(e + ne - k, ne)

            @pl.when(z - d >= 0)
            def _():
                hop(z - d, s, 0, up_sem).wait_recv()
                forward_up(z - d, s)

            @pl.when(z + d < nd)
            def _():
                hop(z + d, s, 0, up_sem).wait_recv()
                forward_dn(z + d, s)

            compute_ring(d - 1, k)

    @pl.loop(0, ne)
    def _(k):
        compute_ring(nd - 1, k)

    @pl.loop(1, ne)
    def _(k):
        cross(lax.rem(e + k, ne)).wait_send()

    @pl.loop(0, nd)
    def _(o):
        @pl.loop(0, ne)
        def _(s):
            @pl.when((z < nd - 1) & (o <= z))
            def _():
                hop(o, s, 0, up_sem).wait_send()

            @pl.when((z > 0) & (o >= z))
            def _():
                hop(o, s, 0, dn_sem).wait_send()


def dispatch(buffer, weights, nd, ne):
    _, height, width = buffer.shape
    hidden = weights.shape[1]
    return pl.pallas_call(
        functools.partial(dispatch_kernel, nd, ne),
        out_shape=(
            jax.ShapeDtypeStruct((nd, ne, height, width), buffer.dtype),
            jax.ShapeDtypeStruct((nd, ne * height, hidden), jnp.bfloat16),
            jax.ShapeDtypeStruct((nd, ne * height, hidden), jnp.float32),
        ),
        in_specs=[vmem(), vmem()],
        out_specs=(vmem(), vmem(), vmem()),
        scratch_shapes=[
            pltpu.SemaphoreType.DMA,
            pltpu.SemaphoreType.DMA((ne,)),
            pltpu.SemaphoreType.DMA((nd, ne)),
            pltpu.SemaphoreType.DMA((nd, ne)),
            pltpu.SemaphoreType.DMA((nd, ne)),
        ],
        compiler_params=pltpu.CompilerParams(has_side_effects=True),
        name="dispatch",
    )(buffer, weights)


def bring_kernel(
    nd,
    ne,
    b_ref,
    x_ref,
    dpre_ref,
    a_ref,
    d_ref,
    ret_ref,
    gup_ref,
    gdn_ref,
    from_dn,
    from_up,
    fin,
    up_sem,
    dn_sem,
    ru_sem,
    rd_sem,
    a_sem,
    ra_sem,
):
    window = min(4, ne)
    z = lax.axis_index("dp")
    e = lax.axis_index("expert")

    def rise(src, o, s):
        return pltpu.make_async_remote_copy(
            src_ref=src.at[o, s],
            dst_ref=from_dn.at[o, s],
            send_sem=up_sem.at[o, s],
            recv_sem=ru_sem.at[o, s],
            device_id=(z + 1, e),
            device_id_type=MESH,
        )

    def fall(src, o, s):
        return pltpu.make_async_remote_copy(
            src_ref=src.at[o, s],
            dst_ref=from_up.at[o, s],
            send_sem=dn_sem.at[o, s],
            recv_sem=rd_sem.at[o, s],
            device_id=(z - 1, e),
            device_id_type=MESH,
        )

    def cross(s):
        return pltpu.make_async_remote_copy(
            src_ref=fin.at[s],
            dst_ref=ret_ref.at[e],
            send_sem=a_sem.at[s],
            recv_sem=ra_sem.at[e],
            device_id=(z, s),
            device_id_type=MESH,
        )

    def back(s):
        return pltpu.make_async_remote_copy(
            src_ref=fin.at[s],
            dst_ref=ret_ref.at[s],
            send_sem=a_sem.at[s],
            recv_sem=ra_sem.at[s],
            device_id=(z, s),
            device_id_type=MESH,
        )

    def place(t):
        return lax.rem(e + lax.rem(t, ne) + 1, ne)

    def risen(t):
        rise(b_ref, nd - 1 - t // ne, place(t)).wait_send()

    def fallen(t):
        fall(b_ref, t // ne, place(t)).wait_send()

    def weights(left, right, out, k):
        tiles = left.shape[1] // 128
        every = ne // tiles

        @pl.when(lax.rem(k, every) == 0)
        def _():
            cols = pl.ds(pl.multiple_of(k // every * 128, 128), 128)
            out[cols, :] = lax.dot_general(
                left[:, cols],
                right[...],
                (((0,), (0,)), ((), ())),
                preferred_element_type=jnp.float32,
            )

    def add(held, o, s):
        total = held[o, s].astype(jnp.float32) + b_ref[o, s].astype(jnp.float32)
        held[o, s] = total.astype(held.dtype)

    for j in range(nd - 1):
        high, low = nd - 1 - j, j

        @pl.loop(0, ne)
        def _(k):
            s = lax.rem(e + k + 1, ne)
            t = j * ne + k

            @pl.when((high > z) & (t >= window))
            def _():
                risen(t - window)

            @pl.when((low < z) & (t >= window))
            def _():
                fallen(t - window)

            @pl.when((high > z) & (z == 0))
            def _():
                rise(b_ref, high, s).start()

            @pl.when((high > z) & (z > 0))
            def _():
                rise(from_dn, high, s).wait_recv()
                add(from_dn, high, s)
                rise(from_dn, high, s).start()

            @pl.when((low < z) & (z == nd - 1))
            def _():
                fall(b_ref, low, s).start()

            @pl.when((low < z) & (z < nd - 1))
            def _():
                fall(from_up, low, s).wait_recv()
                add(from_up, low, s)
                fall(from_up, low, s).start()

            if j == 0:
                weights(x_ref, dpre_ref, gup_ref, k)
            if j == min(1, nd - 2):
                weights(a_ref, d_ref, gdn_ref, k)

    @pl.loop(0, ne)
    def _(k):
        s = lax.rem(e + k + 1, ne)
        fin[s] = b_ref[z, s]

        @pl.when(z > 0)
        def _():
            rise(from_dn, z, s).wait_recv()
            fin[s] = (fin[s].astype(jnp.float32) + from_dn[z, s].astype(jnp.float32)).astype(
                fin.dtype
            )

        @pl.when(z < nd - 1)
        def _():
            fall(from_up, z, s).wait_recv()
            fin[s] = (fin[s].astype(jnp.float32) + from_up[z, s].astype(jnp.float32)).astype(
                fin.dtype
            )

        @pl.when(s != e)
        def _():
            cross(s).start()

        @pl.when(s == e)
        def _():
            ret_ref[e] = fin[e]

    @pl.loop(1, ne)
    def _(k):
        back(lax.rem(e + ne - k, ne)).wait_recv()

    @pl.loop(1, ne)
    def _(k):
        cross(lax.rem(e + k, ne)).wait_send()

    @pl.loop(0, window)
    def _(i):
        @pl.when(z < nd - 1)
        def _():
            risen((nd - 1 - z) * ne - window + i)

        @pl.when(z > 0)
        def _():
            fallen(z * ne - window + i)


def bring_back(partial_rows, xe, dpre, a, d, nd, ne):
    _, _, height, width = partial_rows.shape
    dtype = partial_rows.dtype
    dma = pltpu.SemaphoreType.DMA
    return pl.pallas_call(
        functools.partial(bring_kernel, nd, ne),
        out_shape=(
            jax.ShapeDtypeStruct((ne, height, width), dtype),
            jax.ShapeDtypeStruct((xe.shape[1], dpre.shape[1]), jnp.float32),
            jax.ShapeDtypeStruct((a.shape[1], d.shape[1]), jnp.float32),
        ),
        in_specs=[vmem()] * 5,
        out_specs=(vmem(), vmem(), vmem()),
        scratch_shapes=[
            pltpu.VMEM((nd, ne, height, width), dtype),
            pltpu.VMEM((nd, ne, height, width), dtype),
            pltpu.VMEM((ne, height, width), dtype),
            dma((nd, ne)),
            dma((nd, ne)),
            dma((nd, ne)),
            dma((nd, ne)),
            dma((ne,)),
            dma((ne,)),
        ],
        compiler_params=pltpu.CompilerParams(has_side_effects=True),
        name="bring_back",
    )(partial_rows, xe, dpre, a, d)


def spread(nd, ne, me, src, dst, send_sem, recv_sem):
    n = nd * ne

    def copy(t, sender):
        return pltpu.make_async_remote_copy(
            src_ref=src(t),
            dst_ref=dst.at[sender],
            send_sem=send_sem.at[t],
            recv_sem=recv_sem.at[sender],
            device_id=(t // ne, lax.rem(t, ne)),
            device_id_type=MESH,
        )

    @pl.loop(1, n)
    def _(k):
        copy(lax.rem(me + k, n), me).start()

    @pl.loop(1, n)
    def _(k):
        t = lax.rem(me + n - k, n)
        copy(t, t).wait_recv()

    return copy


def drain(n, me, copy):
    @pl.loop(1, n)
    def _(k):
        copy(lax.rem(me + k, n), me).wait_send()


def pairs_kernel(nd, ne, m_ref, x_ref, out_ref, held, own, s1, r1, s2, r2):
    n = nd * ne
    me = lax.axis_index("dp") * ne + lax.axis_index("expert")
    held[me] = m_ref[me]
    first = spread(nd, ne, me, lambda t: m_ref.at[t], held, s1, r1)
    total = jnp.sum(held[...], axis=0) + x_ref[...]
    own[...] = total
    out_ref[me] = total
    second = spread(nd, ne, me, lambda t: own, out_ref, s2, r2)
    drain(n, me, first)
    drain(n, me, second)


def pair_sums(m, x, nd, ne):
    n = nd * ne
    dma = pltpu.SemaphoreType.DMA
    return pl.pallas_call(
        functools.partial(pairs_kernel, nd, ne),
        out_shape=jax.ShapeDtypeStruct(m.shape, m.dtype),
        in_specs=[vmem(), vmem()],
        out_specs=vmem(),
        scratch_shapes=[
            pltpu.VMEM(m.shape, m.dtype),
            pltpu.VMEM(x.shape, x.dtype),
            dma((n,)),
            dma((n,)),
            dma((n,)),
            dma((n,)),
        ],
        compiler_params=pltpu.CompilerParams(has_side_effects=True),
        name="pair_sums",
    )(m, x)


def everyone_kernel(nd, ne, x_ref, out_ref, s1, r1):
    n = nd * ne
    me = lax.axis_index("dp") * ne + lax.axis_index("expert")
    out_ref[me] = x_ref[...]
    drain(n, me, spread(nd, ne, me, lambda t: x_ref, out_ref, s1, r1))


def everyone(x, nd, ne):
    n = nd * ne
    dma = pltpu.SemaphoreType.DMA
    return pl.pallas_call(
        functools.partial(everyone_kernel, nd, ne),
        out_shape=jax.ShapeDtypeStruct((n,) + x.shape, x.dtype),
        in_specs=[vmem()],
        out_specs=vmem(),
        scratch_shapes=[dma((n,)), dma((n,))],
        compiler_params=pltpu.CompilerParams(has_side_effects=True),
        name="everyone",
    )(x)


def body(
    tokens,
    expert_ids,
    caption_lengths,
    layer_norm_gain,
    router,
    w_up,
    w_down,
    logit_scale,
    logit_bias,
):
    nd = lax.axis_size("dp")
    ne = lax.axis_size("expert")
    n = nd * ne
    assert tokens.shape[0] == 1 and w_up.shape[0] == 1
    rows = SEQ
    experts = router.shape[1]
    slots = rows * 4 // (3 * experts) + 1
    height = -(-(slots + 1) // 8) * 8
    total = n * height
    expert = lax.axis_index("expert")
    me = lax.axis_index("dp") * ne + expert
    wu, wd = w_up[0], w_down[0]

    x = tokens.reshape(rows, D).astype(jnp.float32)
    mean = jnp.mean(x, axis=1, keepdims=True)
    var = jnp.mean((x - mean) ** 2, axis=1, keepdims=True)
    rstd = 1.0 / jnp.sqrt(var + eps)
    xhat = (x - mean) * rstd
    xn = (xhat * layer_norm_gain).astype(jnp.bfloat16)

    ids = expert_ids.reshape(rows)
    onehot = ids[:, None] == jnp.arange(experts, dtype=jnp.int32)[None, :]
    earlier = jnp.arange(rows)[:, None] > jnp.arange(rows)[None, :]
    before = dot(earlier.astype(jnp.bfloat16), onehot.astype(jnp.bfloat16), ((1,), (0,)))
    slot = jnp.sum(jnp.where(onehot, before, 0.0), axis=1).astype(jnp.int32)
    dest = ids * height + slot
    place = (jnp.arange(experts * height, dtype=jnp.int32)[:, None] == dest[None, :]).astype(
        jnp.bfloat16
    )
    length = caption_lengths.astype(jnp.float32)
    row = jnp.arange(rows, dtype=jnp.int32)
    mark = jnp.where(row < PATCH, -1.0, jnp.where(row - PATCH < caption_lengths[0], length[0], 0.0))
    marks = jnp.sum(place.astype(jnp.float32) * mark[None, :], axis=1).reshape(experts, 1, height)
    marks = jnp.pad(marks, ((0, 0), (0, 0), (0, D - height)))
    packed = dot(place, xn, ((1,), (0,))).reshape(experts, height, D)
    is_mark = (jnp.arange(height) == slots)[None, :, None]
    packed = jnp.where(is_mark, marks, packed).astype(jnp.bfloat16)

    got, act, slope = dispatch(packed, wu, nd, ne)
    act, slope = act.reshape(total, -1), slope.reshape(total, -1)
    xe = got.reshape(total, D)

    marks = got.reshape(n, height, D)[:, slots, :height].astype(jnp.float32)
    marks = jnp.where(jnp.arange(height)[None, :] < slots, marks, 0.0).reshape(total)
    is_img, is_txt = marks < 0.0, marks > 0.0
    weight = jnp.where(is_img, 1.0 / PATCH, jnp.where(is_txt, 1.0 / jnp.maximum(marks, 1.0), 0.0))
    column = lax.dynamic_slice_in_dim(router, expert, 1, axis=1)
    columns = jnp.concatenate(split3(column), axis=1)
    gate = jax.nn.sigmoid(jnp.sum(dot(xe, columns, ((1,), (0,))), axis=1))
    coef_row = weight * gate
    kind = jnp.arange(2 * n, dtype=jnp.int32)[:, None]
    pair_of = jnp.arange(total, dtype=jnp.int32)[None, :] // height
    member = (kind // 2 == pair_of) & ((kind % 2 == 0) == is_img[None, :])
    q_high, q_low = split(jnp.where(member, coef_row[None, :], 0.0))
    both = dot(jnp.concatenate([q_high, q_low], axis=0), act, ((1,), (0,)))
    a = both[: 2 * n] + both[2 * n :]
    a_high, a_low = split(a)
    both = dot(jnp.concatenate([a_high, a_low], axis=0), wd, ((1,), (0,)))
    moe_sums = both[: 2 * n] + both[2 * n :]

    img_x = jnp.sum(x[:PATCH], axis=0) / PATCH
    mask = (jnp.arange(CAPLEN, dtype=jnp.int32) < caption_lengths[0]).astype(jnp.float32)
    txt_x = jnp.sum(x[PATCH:] * mask[:, None], axis=0) / length[0]
    own_x = jnp.concatenate([img_x, txt_x]).reshape(8, 2 * D // 8)
    sums = pair_sums(moe_sums.reshape(n, 8, 2 * D // 8), own_x, nd, ne).reshape(n, 2, D)
    img, txt = sums[:, 0], sums[:, 1]

    ru = jnp.sqrt(jnp.mean(img * img, axis=1, keepdims=True) + eps)
    rv = jnp.sqrt(jnp.mean(txt * txt, axis=1, keepdims=True) + eps)
    u, v = img / ru, txt / rv
    scale = logit_scale[0]
    logits = (
        scale * lax.dot_general(u, v, (((1,), (1,)), ((), ())), precision=HIGHEST) / D
        + logit_bias[0]
    )
    sign = 2.0 * jnp.eye(n, dtype=jnp.float32) - 1.0
    loss = -jnp.sum(jax.nn.log_sigmoid(sign * logits)) / n
    coef = -(loss_scale / n) * sign * jax.nn.sigmoid(-sign * logits)
    du = scale / D * jnp.dot(coef, v, precision=HIGHEST)
    dv = scale / D * lax.dot_general(coef, u, (((0,), (0,)), ((), ())), precision=HIGHEST)
    dimg = (du - u * jnp.mean(du * u, axis=1, keepdims=True)) / ru
    dtxt = (dv - v * jnp.mean(dv * v, axis=1, keepdims=True)) / rv
    dvec = jnp.stack([dimg, dtxt], axis=1).reshape(2 * n, D)
    d_high, d_low = split(dvec)

    both = dot(jnp.concatenate([d_high, d_low], axis=0), wd, ((1,), (1,)))
    dhid = both[: 2 * n] + both[2 * n :]
    h_high, h_low = split(dhid)
    both = dot(act, jnp.concatenate([h_high, h_low], axis=0), ((1,), (1,)))
    products = jnp.where(member.T, both[:, : 2 * n] + both[:, 2 * n :], 0.0)
    dgl = jnp.sum(products, axis=1) * weight * gate * (1.0 - gate)
    ones = member.T.astype(jnp.bfloat16)
    chosen = dot(
        jnp.concatenate([ones, ones], axis=1),
        jnp.concatenate([h_high, h_low], axis=0),
        ((1,), (0,)),
    )
    dpre = (coef_row[:, None] * chosen * slope).astype(jnp.bfloat16)
    back = (dot(dpre, wu, ((1,), (1,))) + dgl[:, None] * column[:, 0][None, :]).astype(jnp.bfloat16)
    returned, grad_up, grad_down = bring_back(
        back.reshape(nd, ne, height, D),
        xe,
        dpre,
        jnp.concatenate([a_high, a_high, a_low], axis=0),
        jnp.concatenate([d_high, d_low, d_high], axis=0),
        nd,
        ne,
    )
    grad_up, grad_down = grad_up[None], grad_down[None]
    router_part = jnp.sum(dot(jnp.stack(split3(dgl)), xe, ((1,), (0,))), axis=0)

    dxn = dot(place, returned.reshape(experts * height, D), ((0,), (0,)))
    gain_part = jnp.sum(dxn * xhat, axis=0)
    g = dxn * layer_norm_gain
    normed = (
        g - jnp.mean(g, axis=1, keepdims=True) - xhat * jnp.mean(g * xhat, axis=1, keepdims=True)
    ) * rstd
    mine = lax.dynamic_slice_in_dim(dvec, 2 * me, 2, axis=0)
    dy = jnp.where(
        (row < PATCH)[:, None],
        mine[0:1] / PATCH,
        jnp.where(mark > 0.0, 1.0 / length[0], 0.0)[:, None] * mine[1:2],
    )
    grad_tokens = (dy + normed).astype(jnp.bfloat16).reshape(1, SEQ, D)
    last = everyone(jnp.concatenate([gain_part, router_part]).reshape(8, 2 * D // 8), nd, ne)
    last = last.reshape(nd, ne, 2, D)
    gain_grad = jnp.sum(last[:, :, 0], axis=(0, 1))
    grad_router = jnp.sum(last[:, :, 1], axis=0).T
    return (loss.reshape(1), grad_tokens, grad_up, grad_down, grad_router, gain_grad)


def solution(mesh):
    return jax.shard_map(
        body,
        mesh=mesh,
        in_specs=(
            P(("dp", "expert"), None, None),
            P(("dp", "expert"), None, None),
            P(("dp", "expert")),
            P(),
            P(),
            P("expert", None, "dp"),
            P("expert", "dp", None),
            P(),
            P(),
        ),
        out_specs=(
            P(),
            P(("dp", "expert"), None, None),
            P("expert", None, "dp"),
            P("expert", "dp", None),
            P(),
            P(),
        ),
        check_vma=False,
    )
```

```python
import functools

import jax
import jax.numpy as jnp
from jax import lax
from jax.experimental import pallas as pl
from jax.experimental.pallas import tpu as pltpu
from jax.sharding import PartitionSpec as P

D = 1024
PATCH = 196
CAPLEN = 16
SEQ = 212

eps = 1e-06
loss_scale = 1024.0
MESH = pl.DeviceIdType.MESH
HIGHEST = lax.Precision.HIGHEST


def split(value):
    high = lax.reduce_precision(value, 8, 7)
    return high.astype(jnp.bfloat16), (value - high).astype(jnp.bfloat16)


def split3(value):
    high = lax.reduce_precision(value, 8, 7)
    return (high.astype(jnp.bfloat16),) + split(value - high)


def dot(a, b, contract):
    return lax.dot_general(a, b, (contract, ((), ())), preferred_element_type=jnp.float32)


def vmem():
    return pl.BlockSpec(memory_space=pltpu.VMEM)


def dispatch_kernel(
    nd, ne, x_ref, w_ref, out_ref, act_ref, slope_ref, own_sem, a_sem, up_sem, dn_sem, r_sem
):
    _, height, width = x_ref.shape
    hidden = w_ref.shape[1]
    tiles = hidden // 128
    every = ne // tiles
    z = lax.axis_index("dp")
    e = lax.axis_index("expert")

    def hop(o, s, step, sem):
        return pltpu.make_async_remote_copy(
            src_ref=out_ref.at[o, s],
            dst_ref=out_ref.at[o, s],
            send_sem=sem.at[o, s],
            recv_sem=r_sem.at[o, s],
            device_id=(z + step, e),
            device_id_type=MESH,
        )

    def cross(t):
        return pltpu.make_async_remote_copy(
            src_ref=x_ref.at[t],
            dst_ref=out_ref.at[z, e],
            send_sem=a_sem.at[t],
            recv_sem=r_sem.at[z, e],
            device_id=(z, t),
            device_id_type=MESH,
        )

    def forward_up(o, s):
        @pl.when(z < nd - 1)
        def _():
            hop(o, s, 1, up_sem).start()

    def forward_dn(o, s):
        @pl.when(z > 0)
        def _():
            hop(o, s, -1, dn_sem).start()

    def compute(o, k):
        cols = pl.ds(pl.multiple_of(k // every * 128, 128), 128)
        xe = out_ref[o].reshape(ne * height, width)
        pre = jnp.dot(xe, w_ref[:, cols], preferred_element_type=jnp.float32)
        half = 0.5 * (1.0 + lax.erf(pre * 0.7071067811865476))
        bell = jnp.exp(-0.5 * pre * pre) * 0.3989422804014327
        act_ref[o, :, cols] = (pre * half).astype(jnp.bfloat16)
        slope_ref[o, :, cols] = half + pre * bell

    def compute_ring(d, k):
        @pl.when(lax.rem(k, every) == 0)
        def _():
            @pl.when(z - d >= 0)
            def _():
                compute(z - d, k)

            if d > 0:

                @pl.when(z + d < nd)
                def _():
                    compute(z + d, k)

    own = pltpu.make_async_copy(x_ref.at[e], out_ref.at[z, e], own_sem)
    own.start()

    @pl.loop(1, ne)
    def _(k):
        cross(lax.rem(e + k, ne)).start()

    own.wait()
    forward_up(z, e)
    forward_dn(z, e)

    @pl.loop(1, ne)
    def _(k):
        s = lax.rem(e + ne - k, ne)
        hop(z, s, 0, up_sem).wait_recv()
        forward_up(z, s)
        forward_dn(z, s)

    for d in range(1, nd):

        @pl.loop(0, ne)
        def _(k):
            s = lax.rem(e + ne - k, ne)

            @pl.when(z - d >= 0)
            def _():
                hop(z - d, s, 0, up_sem).wait_recv()
                forward_up(z - d, s)

            @pl.when(z + d < nd)
            def _():
                hop(z + d, s, 0, up_sem).wait_recv()
                forward_dn(z + d, s)

            compute_ring(d - 1, k)

    @pl.loop(0, ne)
    def _(k):
        compute_ring(nd - 1, k)

    @pl.loop(1, ne)
    def _(k):
        cross(lax.rem(e + k, ne)).wait_send()

    @pl.loop(0, nd)
    def _(o):
        @pl.loop(0, ne)
        def _(s):
            @pl.when((z < nd - 1) & (o <= z))
            def _():
                hop(o, s, 0, up_sem).wait_send()

            @pl.when((z > 0) & (o >= z))
            def _():
                hop(o, s, 0, dn_sem).wait_send()


def dispatch(buffer, weights, nd, ne):
    _, height, width = buffer.shape
    hidden = weights.shape[1]
    return pl.pallas_call(
        functools.partial(dispatch_kernel, nd, ne),
        out_shape=(
            jax.ShapeDtypeStruct((nd, ne, height, width), buffer.dtype),
            jax.ShapeDtypeStruct((nd, ne * height, hidden), jnp.bfloat16),
            jax.ShapeDtypeStruct((nd, ne * height, hidden), jnp.float32),
        ),
        in_specs=[vmem(), vmem()],
        out_specs=(vmem(), vmem(), vmem()),
        scratch_shapes=[
            pltpu.SemaphoreType.DMA,
            pltpu.SemaphoreType.DMA((ne,)),
            pltpu.SemaphoreType.DMA((nd, ne)),
            pltpu.SemaphoreType.DMA((nd, ne)),
            pltpu.SemaphoreType.DMA((nd, ne)),
        ],
        compiler_params=pltpu.CompilerParams(has_side_effects=True),
        name="dispatch",
    )(buffer, weights)


def bring_kernel(
    nd,
    ne,
    x_ref,
    slope_ref,
    w_ref,
    q_ref,
    h_ref,
    c_ref,
    a_ref,
    d_ref,
    rp_ref,
    ret_ref,
    gup_ref,
    gdn_ref,
    rall_ref,
    b_ref,
    dpre_ref,
    from_dn,
    from_up,
    up_sem,
    dn_sem,
    ru_sem,
    rd_sem,
    a_sem,
    ra_sem,
    rs_sem,
    rr_sem,
):
    _, _, height, width = b_ref.shape
    plane = ne * height
    window = min(4, ne)
    lag = min(4, ne)
    z = lax.axis_index("dp")
    e = lax.axis_index("expert")
    me = z * ne + e
    rall_ref[me] = rp_ref[...]
    router_arrive, router_drain = spread(nd, ne, me, lambda t: rp_ref, rall_ref, rs_sem, rr_sem)

    def produce(o):
        part = pl.ds(o * plane, plane)
        dact = jnp.dot(q_ref[part, :], h_ref[o], preferred_element_type=jnp.float32)
        dpre = (dact * slope_ref[part, :]).astype(jnp.bfloat16)
        dpre_ref[part, :] = dpre
        back = lax.dot_general(
            dpre, w_ref[...], (((1,), (1,)), ((), ())), preferred_element_type=jnp.float32
        )
        back += jnp.dot(q_ref[part, :], c_ref[...], preferred_element_type=jnp.float32)
        b_ref[o] = back.astype(jnp.bfloat16).reshape(ne, height, width)

    def rise(src, o, s):
        return pltpu.make_async_remote_copy(
            src_ref=src.at[o, s],
            dst_ref=from_dn.at[o, s],
            send_sem=up_sem.at[o, s],
            recv_sem=ru_sem.at[o, s],
            device_id=(z + 1, e),
            device_id_type=MESH,
        )

    def fall(src, o, s):
        return pltpu.make_async_remote_copy(
            src_ref=src.at[o, s],
            dst_ref=from_up.at[o, s],
            send_sem=dn_sem.at[o, s],
            recv_sem=rd_sem.at[o, s],
            device_id=(z - 1, e),
            device_id_type=MESH,
        )

    def cross(s):
        return pltpu.make_async_remote_copy(
            src_ref=b_ref.at[z, s],
            dst_ref=ret_ref.at[e],
            send_sem=a_sem.at[s],
            recv_sem=ra_sem.at[e],
            device_id=(z, s),
            device_id_type=MESH,
        )

    def back(s):
        return pltpu.make_async_remote_copy(
            src_ref=b_ref.at[z, s],
            dst_ref=ret_ref.at[s],
            send_sem=a_sem.at[s],
            recv_sem=ra_sem.at[s],
            device_id=(z, s),
            device_id_type=MESH,
        )

    def place(t):
        return lax.rem(e + lax.rem(t, ne) + 1, ne)

    def risen(t):
        rise(b_ref, nd - 1 - t // ne, place(t)).wait_send()

    def fallen(t):
        fall(b_ref, t // ne, place(t)).wait_send()

    def weights(left, right, out, k):
        tiles = left.shape[1] // 128
        every = ne // tiles

        @pl.when(lax.rem(k, every) == 0)
        def _():
            cols = pl.ds(pl.multiple_of(k // every * 128, 128), 128)
            out[cols, :] = lax.dot_general(
                left[:, cols],
                right[...],
                (((0,), (0,)), ((), ())),
                preferred_element_type=jnp.float32,
            )

    def add(held, other, o, s):
        total = held[o, s].astype(jnp.float32) + other[o, s].astype(jnp.float32)
        held[o, s] = total.astype(held.dtype)

    upper = (z >= nd // 2).astype(jnp.int32)

    def travel(step):
        t_up = step - lag * upper
        t_dn = step - lag * (1 - upper)

        @pl.when((t_up >= 0) & (t_up < (nd - 1 - z) * ne))
        def _():
            o = nd - 1 - t_up // ne
            s = place(t_up)

            @pl.when(t_up >= window)
            def _():
                risen(t_up - window)

            @pl.when(z == 0)
            def _():
                rise(b_ref, o, s).start()

            @pl.when(z > 0)
            def _():
                rise(from_dn, o, s).wait_recv()
                add(from_dn, b_ref, o, s)
                rise(from_dn, o, s).start()

        @pl.when((t_dn >= 0) & (t_dn < z * ne))
        def _():
            o = t_dn // ne
            s = place(t_dn)

            @pl.when(t_dn >= window)
            def _():
                fallen(t_dn - window)

            @pl.when(z == nd - 1)
            def _():
                fall(b_ref, o, s).start()

            @pl.when(z < nd - 1)
            def _():
                fall(from_up, o, s).wait_recv()
                add(from_up, b_ref, o, s)
                fall(from_up, o, s).start()

    for j in range(nd - 1):
        if j <= nd - 1 - j:
            produce(nd - 1 - j)
        if j < nd - 1 - j:
            produce(j)

        @pl.loop(0, ne)
        def _(k):
            travel(j * ne + k)
            if j == min(nd // 2, nd - 2):
                weights(x_ref, dpre_ref, gup_ref, k)
                weights(a_ref, d_ref, gdn_ref, k)

    @pl.loop((nd - 1) * ne, (nd - 1) * ne + lag)
    def _(step):
        travel(step)

    @pl.loop(0, ne)
    def _(k):
        s = lax.rem(e + k + 1, ne)

        @pl.when(z > 0)
        def _():
            rise(from_dn, z, s).wait_recv()
            add(b_ref, from_dn, z, s)

        @pl.when(z < nd - 1)
        def _():
            fall(from_up, z, s).wait_recv()
            add(b_ref, from_up, z, s)

        @pl.when(s != e)
        def _():
            cross(s).start()

        @pl.when(s == e)
        def _():
            ret_ref[e] = b_ref[z, e]

    @pl.loop(1, ne)
    def _(k):
        back(lax.rem(e + ne - k, ne)).wait_recv()

    @pl.loop(1, ne)
    def _(k):
        cross(lax.rem(e + k, ne)).wait_send()

    @pl.loop(0, window)
    def _(i):
        @pl.when(z < nd - 1)
        def _():
            risen((nd - 1 - z) * ne - window + i)

        @pl.when(z > 0)
        def _():
            fallen(z * ne - window + i)

    router_arrive()
    router_drain()

def bring_back(xe, slope, weights, q, h, c, a, d, router_part, nd, ne):
    total, width = xe.shape
    hidden = slope.shape[1]
    n = nd * ne
    height = total // n
    dtype = jnp.bfloat16
    dma = pltpu.SemaphoreType.DMA
    return pl.pallas_call(
        functools.partial(bring_kernel, nd, ne),
        out_shape=(
            jax.ShapeDtypeStruct((ne, height, width), dtype),
            jax.ShapeDtypeStruct((width, hidden), jnp.float32),
            jax.ShapeDtypeStruct((hidden, width), jnp.float32),
            jax.ShapeDtypeStruct((n,) + router_part.shape, jnp.float32),
        ),
        in_specs=[vmem()] * 9,
        out_specs=(vmem(),) * 4,
        scratch_shapes=[
            pltpu.VMEM((nd, ne, height, width), dtype),
            pltpu.VMEM((total, hidden), dtype),
            pltpu.VMEM((nd, ne, height, width), dtype),
            pltpu.VMEM((nd, ne, height, width), dtype),
            dma((nd, ne)),
            dma((nd, ne)),
            dma((nd, ne)),
            dma((nd, ne)),
            dma((ne,)),
            dma((ne,)),
            dma((n,)),
            dma((n,)),
        ],
        compiler_params=pltpu.CompilerParams(has_side_effects=True),
        name="bring_back",
    )(xe, slope, weights, q, h, c, a, d, router_part)


def spread(nd, ne, me, src, dst, send_sem, recv_sem):
    n = nd * ne

    def copy(t, sender):
        return pltpu.make_async_remote_copy(
            src_ref=src(t),
            dst_ref=dst.at[sender],
            send_sem=send_sem.at[t],
            recv_sem=recv_sem.at[sender],
            device_id=(t // ne, lax.rem(t, ne)),
            device_id_type=MESH,
        )

    @pl.loop(1, n)
    def _(k):
        copy(lax.rem(me + k, n), me).start()

    def arrive():
        @pl.loop(1, n)
        def _(k):
            t = lax.rem(me + n - k, n)
            copy(t, t).wait_recv()

    def drain():
        @pl.loop(1, n)
        def _(k):
            copy(lax.rem(me + k, n), me).wait_send()

    return arrive, drain


def pairs_kernel(nd, ne, m_ref, x_ref, out_ref, held, own, s1, r1, s2, r2):
    me = lax.axis_index("dp") * ne + lax.axis_index("expert")
    held[me] = m_ref[me]
    arrive, drain_first = spread(nd, ne, me, lambda t: m_ref.at[t], held, s1, r1)
    arrive()
    total = jnp.sum(held[...], axis=0) + x_ref[...]
    own[...] = total
    out_ref[me] = total
    arrive, drain_second = spread(nd, ne, me, lambda t: own, out_ref, s2, r2)
    arrive()
    drain_first()
    drain_second()


def pair_sums(m, x, nd, ne):
    n = nd * ne
    dma = pltpu.SemaphoreType.DMA
    return pl.pallas_call(
        functools.partial(pairs_kernel, nd, ne),
        out_shape=jax.ShapeDtypeStruct(m.shape, m.dtype),
        in_specs=[vmem(), vmem()],
        out_specs=vmem(),
        scratch_shapes=[
            pltpu.VMEM(m.shape, m.dtype),
            pltpu.VMEM(x.shape, x.dtype),
            dma((n,)),
            dma((n,)),
            dma((n,)),
            dma((n,)),
        ],
        compiler_params=pltpu.CompilerParams(has_side_effects=True),
        name="pair_sums",
    )(m, x)


def everyone_kernel(nd, ne, x_ref, out_ref, s1, r1):
    me = lax.axis_index("dp") * ne + lax.axis_index("expert")
    out_ref[me] = x_ref[...]
    arrive, drain = spread(nd, ne, me, lambda t: x_ref, out_ref, s1, r1)
    arrive()
    drain()


def everyone(x, nd, ne):
    n = nd * ne
    dma = pltpu.SemaphoreType.DMA
    return pl.pallas_call(
        functools.partial(everyone_kernel, nd, ne),
        out_shape=jax.ShapeDtypeStruct((n,) + x.shape, x.dtype),
        in_specs=[vmem()],
        out_specs=vmem(),
        scratch_shapes=[dma((n,)), dma((n,))],
        compiler_params=pltpu.CompilerParams(has_side_effects=True),
        name="everyone",
    )(x)


def body(
    tokens,
    expert_ids,
    caption_lengths,
    layer_norm_gain,
    router,
    w_up,
    w_down,
    logit_scale,
    logit_bias,
):
    nd = lax.axis_size("dp")
    ne = lax.axis_size("expert")
    n = nd * ne
    assert tokens.shape[0] == 1 and w_up.shape[0] == 1
    rows = SEQ
    experts = router.shape[1]
    slots = rows * 4 // (3 * experts) + 1
    height = -(-(slots + 1) // 8) * 8
    total = n * height
    expert = lax.axis_index("expert")
    me = lax.axis_index("dp") * ne + expert
    wu, wd = w_up[0], w_down[0]

    x = tokens.reshape(rows, D).astype(jnp.float32)
    mean = jnp.mean(x, axis=1, keepdims=True)
    var = jnp.mean((x - mean) ** 2, axis=1, keepdims=True)
    rstd = 1.0 / jnp.sqrt(var + eps)
    xhat = (x - mean) * rstd
    xn = (xhat * layer_norm_gain).astype(jnp.bfloat16)

    ids = expert_ids.reshape(rows)
    onehot = ids[:, None] == jnp.arange(experts, dtype=jnp.int32)[None, :]
    earlier = jnp.arange(rows)[:, None] > jnp.arange(rows)[None, :]
    before = dot(earlier.astype(jnp.bfloat16), onehot.astype(jnp.bfloat16), ((1,), (0,)))
    slot = jnp.sum(jnp.where(onehot, before, 0.0), axis=1).astype(jnp.int32)
    dest = ids * height + slot
    place = (jnp.arange(experts * height, dtype=jnp.int32)[:, None] == dest[None, :]).astype(
        jnp.bfloat16
    )
    length = caption_lengths.astype(jnp.float32)
    row = jnp.arange(rows, dtype=jnp.int32)
    mark = jnp.where(row < PATCH, -1.0, jnp.where(row - PATCH < caption_lengths[0], length[0], 0.0))
    marks = jnp.sum(place.astype(jnp.float32) * mark[None, :], axis=1).reshape(experts, 1, height)
    marks = jnp.pad(marks, ((0, 0), (0, 0), (0, D - height)))
    packed = dot(place, xn, ((1,), (0,))).reshape(experts, height, D)
    is_mark = (jnp.arange(height) == slots)[None, :, None]
    packed = jnp.where(is_mark, marks, packed).astype(jnp.bfloat16)

    got, act, slope = dispatch(packed, wu, nd, ne)
    act, slope = act.reshape(total, -1), slope.reshape(total, -1)
    xe = got.reshape(total, D)

    marks = got.reshape(n, height, D)[:, slots, :height].astype(jnp.float32)
    marks = jnp.where(jnp.arange(height)[None, :] < slots, marks, 0.0).reshape(total)
    is_img, is_txt = marks < 0.0, marks > 0.0
    weight = jnp.where(is_img, 1.0 / PATCH, jnp.where(is_txt, 1.0 / jnp.maximum(marks, 1.0), 0.0))
    column = lax.dynamic_slice_in_dim(router, expert, 1, axis=1)
    columns = jnp.concatenate(split3(column), axis=1)
    gate = jax.nn.sigmoid(jnp.sum(dot(xe, columns, ((1,), (0,))), axis=1))
    coef_row = weight * gate
    kind = jnp.arange(2 * n, dtype=jnp.int32)[:, None]
    pair_of = jnp.arange(total, dtype=jnp.int32)[None, :] // height
    member = (kind // 2 == pair_of) & ((kind % 2 == 0) == is_img[None, :])
    q_high, q_low = split(jnp.where(member, coef_row[None, :], 0.0))
    both = dot(jnp.concatenate([q_high, q_low], axis=0), act, ((1,), (0,)))
    a = both[: 2 * n] + both[2 * n :]
    a_high, a_low = split(a)
    both = dot(jnp.concatenate([a_high, a_low], axis=0), wd, ((1,), (0,)))
    moe_sums = both[: 2 * n] + both[2 * n :]

    img_x = jnp.sum(x[:PATCH], axis=0) / PATCH
    mask = (jnp.arange(CAPLEN, dtype=jnp.int32) < caption_lengths[0]).astype(jnp.float32)
    txt_x = jnp.sum(x[PATCH:] * mask[:, None], axis=0) / length[0]
    own_x = jnp.concatenate([img_x, txt_x]).reshape(8, 2 * D // 8)
    sums = pair_sums(moe_sums.reshape(n, 8, 2 * D // 8), own_x, nd, ne).reshape(n, 2, D)
    img, txt = sums[:, 0], sums[:, 1]

    ru = jnp.sqrt(jnp.mean(img * img, axis=1, keepdims=True) + eps)
    rv = jnp.sqrt(jnp.mean(txt * txt, axis=1, keepdims=True) + eps)
    u, v = img / ru, txt / rv
    scale = logit_scale[0]
    logits = (
        scale * lax.dot_general(u, v, (((1,), (1,)), ((), ())), precision=HIGHEST) / D
        + logit_bias[0]
    )
    sign = 2.0 * jnp.eye(n, dtype=jnp.float32) - 1.0
    loss = -jnp.sum(jax.nn.log_sigmoid(sign * logits)) / n
    coef = -(loss_scale / n) * sign * jax.nn.sigmoid(-sign * logits)
    du = scale / D * jnp.dot(coef, v, precision=HIGHEST)
    dv = scale / D * lax.dot_general(coef, u, (((0,), (0,)), ((), ())), precision=HIGHEST)
    dimg = (du - u * jnp.mean(du * u, axis=1, keepdims=True)) / ru
    dtxt = (dv - v * jnp.mean(dv * v, axis=1, keepdims=True)) / rv
    dvec = jnp.stack([dimg, dtxt], axis=1).reshape(2 * n, D)
    d_high, d_low = split(dvec)

    both = dot(jnp.concatenate([d_high, d_low], axis=0), wd, ((1,), (1,)))
    dhid = both[: 2 * n] + both[2 * n :]
    h_high, h_low = split(dhid)
    both = dot(act, jnp.concatenate([h_high, h_low], axis=0), ((1,), (1,)))
    products = jnp.where(member.T, both[:, : 2 * n] + both[:, 2 * n :], 0.0)
    dgl = jnp.sum(products, axis=1) * weight * gate * (1.0 - gate)
    router_part = jnp.sum(dot(jnp.stack(split3(dgl)), xe, ((1,), (0,))), axis=0)
    local = jnp.arange(2 * ne, dtype=jnp.int32)[None, :]
    pair_in_plane = lax.rem(jnp.arange(total, dtype=jnp.int32)[:, None] // height, ne)
    own = (local // 2 == pair_in_plane) & ((local % 2 == 0) == is_img[:, None])
    qt_high, qt_low = split(jnp.where(own, coef_row[:, None], 0.0))
    h_high, h_low = h_high.reshape(nd, 2 * ne, -1), h_low.reshape(nd, 2 * ne, -1)
    g_high, g_low = split(dgl[:, None])
    c_high, c_low = split(column.T)
    returned, grad_up, grad_down, router_all = bring_back(
        xe,
        slope,
        wu,
        jnp.concatenate([qt_high, qt_high, qt_low, g_high, g_high, g_low], axis=1),
        jnp.pad(jnp.concatenate([h_high, h_low, h_high], axis=1), ((0, 0), (0, 3), (0, 0))),
        jnp.pad(jnp.concatenate([c_high, c_low, c_high], axis=0), ((6 * ne, 0), (0, 0))),
        jnp.concatenate([a_high, a_high, a_low], axis=0),
        jnp.concatenate([d_high, d_low, d_high], axis=0),
        router_part.reshape(8, D // 8),
        nd,
        ne,
    )
    grad_up, grad_down = grad_up[None], grad_down[None]

    dxn = dot(place, returned.reshape(experts * height, D), ((0,), (0,)))
    gain_part = jnp.sum(dxn * xhat, axis=0)
    g = dxn * layer_norm_gain
    normed = (
        g - jnp.mean(g, axis=1, keepdims=True) - xhat * jnp.mean(g * xhat, axis=1, keepdims=True)
    ) * rstd
    mine = lax.dynamic_slice_in_dim(dvec, 2 * me, 2, axis=0)
    dy = jnp.where(
        (row < PATCH)[:, None],
        mine[0:1] / PATCH,
        jnp.where(mark > 0.0, 1.0 / length[0], 0.0)[:, None] * mine[1:2],
    )
    grad_tokens = (dy + normed).astype(jnp.bfloat16).reshape(1, SEQ, D)
    gain_grad = jnp.sum(everyone(gain_part.reshape(8, D // 8), nd, ne), axis=0).reshape(D)
    grad_router = jnp.sum(router_all.reshape(nd, ne, D), axis=0).T
    return (loss.reshape(1), grad_tokens, grad_up, grad_down, grad_router, gain_grad)


def solution(mesh):
    return jax.shard_map(
        body,
        mesh=mesh,
        in_specs=(
            P(("dp", "expert"), None, None),
            P(("dp", "expert"), None, None),
            P(("dp", "expert")),
            P(),
            P(),
            P("expert", None, "dp"),
            P("expert", "dp", None),
            P(),
            P(),
        ),
        out_specs=(
            P(),
            P(("dp", "expert"), None, None),
            P("expert", None, "dp"),
            P("expert", "dp", None),
            P(),
            P(),
        ),
        check_vma=False,
    )
```

```python
import functools

import jax
import jax.numpy as jnp
from jax import lax
from jax.experimental import pallas as pl
from jax.experimental.pallas import tpu as pltpu
from jax.sharding import PartitionSpec as P

D = 1024
PATCH = 196
CAPLEN = 16
SEQ = 212

eps = 1e-06
loss_scale = 1024.0
MESH = pl.DeviceIdType.MESH
HIGHEST = lax.Precision.HIGHEST


def split(value):
    high = lax.reduce_precision(value, 8, 7)
    return high.astype(jnp.bfloat16), (value - high).astype(jnp.bfloat16)


def split3(value):
    high = lax.reduce_precision(value, 8, 7)
    return (high.astype(jnp.bfloat16),) + split(value - high)


def dot(a, b, contract):
    return lax.dot_general(a, b, (contract, ((), ())), preferred_element_type=jnp.float32)


def vmem():
    return pl.BlockSpec(memory_space=pltpu.VMEM)


def dispatch_kernel(
    nd, ne, x_ref, w_ref, out_ref, act_ref, slope_ref, own_sem, a_sem, up_sem, dn_sem, r_sem
):
    _, height, width = x_ref.shape
    hidden = w_ref.shape[1]
    tiles = hidden // 128
    every = ne // tiles
    z = lax.axis_index("dp")
    e = lax.axis_index("expert")

    def hop(o, s, step, sem):
        return pltpu.make_async_remote_copy(
            src_ref=out_ref.at[o, s],
            dst_ref=out_ref.at[o, s],
            send_sem=sem.at[o, s],
            recv_sem=r_sem.at[o, s],
            device_id=(z + step, e),
            device_id_type=MESH,
        )

    def cross(t):
        return pltpu.make_async_remote_copy(
            src_ref=x_ref.at[t],
            dst_ref=out_ref.at[z, e],
            send_sem=a_sem.at[t],
            recv_sem=r_sem.at[z, e],
            device_id=(z, t),
            device_id_type=MESH,
        )

    def forward_up(o, s):
        @pl.when(z < nd - 1)
        def _():
            hop(o, s, 1, up_sem).start()

    def forward_dn(o, s):
        @pl.when(z > 0)
        def _():
            hop(o, s, -1, dn_sem).start()

    def compute(o, k):
        cols = pl.ds(pl.multiple_of(k // every * 128, 128), 128)
        xe = out_ref[o].reshape(ne * height, width)
        pre = jnp.dot(xe, w_ref[:, cols], preferred_element_type=jnp.float32)
        half = 0.5 * (1.0 + lax.erf(pre * 0.7071067811865476))
        bell = jnp.exp(-0.5 * pre * pre) * 0.3989422804014327
        act_ref[o, :, cols] = (pre * half).astype(jnp.bfloat16)
        slope_ref[o, :, cols] = half + pre * bell

    def compute_ring(d, k):
        @pl.when(lax.rem(k, every) == 0)
        def _():
            @pl.when(z - d >= 0)
            def _():
                compute(z - d, k)

            if d > 0:

                @pl.when(z + d < nd)
                def _():
                    compute(z + d, k)

    own = pltpu.make_async_copy(x_ref.at[e], out_ref.at[z, e], own_sem)
    own.start()

    @pl.loop(1, ne)
    def _(k):
        cross(lax.rem(e + k, ne)).start()

    own.wait()
    forward_up(z, e)
    forward_dn(z, e)

    @pl.loop(1, ne)
    def _(k):
        s = lax.rem(e + ne - k, ne)
        hop(z, s, 0, up_sem).wait_recv()
        forward_up(z, s)
        forward_dn(z, s)

    for d in range(1, nd):

        @pl.loop(0, ne)
        def _(k):
            s = lax.rem(e + ne - k, ne)

            @pl.when(z - d >= 0)
            def _():
                hop(z - d, s, 0, up_sem).wait_recv()
                forward_up(z - d, s)

            @pl.when(z + d < nd)
            def _():
                hop(z + d, s, 0, up_sem).wait_recv()
                forward_dn(z + d, s)

            compute_ring(d - 1, k)

    @pl.loop(0, ne)
    def _(k):
        compute_ring(nd - 1, k)

    @pl.loop(1, ne)
    def _(k):
        cross(lax.rem(e + k, ne)).wait_send()

    @pl.loop(0, nd)
    def _(o):
        @pl.loop(0, ne)
        def _(s):
            @pl.when((z < nd - 1) & (o <= z))
            def _():
                hop(o, s, 0, up_sem).wait_send()

            @pl.when((z > 0) & (o >= z))
            def _():
                hop(o, s, 0, dn_sem).wait_send()


def dispatch(buffer, weights, nd, ne):
    _, height, width = buffer.shape
    hidden = weights.shape[1]
    return pl.pallas_call(
        functools.partial(dispatch_kernel, nd, ne),
        out_shape=(
            jax.ShapeDtypeStruct((nd, ne, height, width), buffer.dtype),
            jax.ShapeDtypeStruct((nd, ne * height, hidden), jnp.bfloat16),
            jax.ShapeDtypeStruct((nd, ne * height, hidden), jnp.float32),
        ),
        in_specs=[vmem(), vmem()],
        out_specs=(vmem(), vmem(), vmem()),
        scratch_shapes=[
            pltpu.SemaphoreType.DMA,
            pltpu.SemaphoreType.DMA((ne,)),
            pltpu.SemaphoreType.DMA((nd, ne)),
            pltpu.SemaphoreType.DMA((nd, ne)),
            pltpu.SemaphoreType.DMA((nd, ne)),
        ],
        compiler_params=pltpu.CompilerParams(has_side_effects=True),
        name="dispatch",
    )(buffer, weights)


def bring_kernel(
    nd,
    ne,
    x_ref,
    slope_ref,
    w_ref,
    q_ref,
    h_ref,
    c_ref,
    a_ref,
    d_ref,
    rp_ref,
    ret_ref,
    gup_ref,
    gdn_ref,
    rall_ref,
    b_ref,
    dpre_ref,
    from_dn,
    from_up,
    up_sem,
    dn_sem,
    ru_sem,
    rd_sem,
    a_sem,
    ra_sem,
    rs_sem,
    rr_sem,
):
    _, _, height, width = b_ref.shape
    plane = ne * height
    window = min(4, ne)
    lag = min(4, ne)
    z = lax.axis_index("dp")
    e = lax.axis_index("expert")
    me = z * ne + e
    rall_ref[me] = rp_ref[...]
    router_arrive, router_drain = spread(nd, ne, me, lambda t: rp_ref, rall_ref, rs_sem, rr_sem)

    def produce(o):
        part = pl.ds(o * plane, plane)
        dact = jnp.dot(q_ref[part, :], h_ref[o], preferred_element_type=jnp.float32)
        dpre = (dact * slope_ref[part, :]).astype(jnp.bfloat16)
        dpre_ref[part, :] = dpre
        back = lax.dot_general(
            dpre, w_ref[...], (((1,), (1,)), ((), ())), preferred_element_type=jnp.float32
        )
        back += jnp.dot(q_ref[part, :], c_ref[...], preferred_element_type=jnp.float32)
        b_ref[o] = back.astype(jnp.bfloat16).reshape(ne, height, width)

    def rise(src, o, s):
        return pltpu.make_async_remote_copy(
            src_ref=src.at[o, s],
            dst_ref=from_dn.at[o, s],
            send_sem=up_sem.at[o, s],
            recv_sem=ru_sem.at[o, s],
            device_id=(z + 1, e),
            device_id_type=MESH,
        )

    def fall(src, o, s):
        return pltpu.make_async_remote_copy(
            src_ref=src.at[o, s],
            dst_ref=from_up.at[o, s],
            send_sem=dn_sem.at[o, s],
            recv_sem=rd_sem.at[o, s],
            device_id=(z - 1, e),
            device_id_type=MESH,
        )

    def cross(s):
        return pltpu.make_async_remote_copy(
            src_ref=b_ref.at[z, s],
            dst_ref=ret_ref.at[e],
            send_sem=a_sem.at[s],
            recv_sem=ra_sem.at[e],
            device_id=(z, s),
            device_id_type=MESH,
        )

    def back(s):
        return pltpu.make_async_remote_copy(
            src_ref=b_ref.at[z, s],
            dst_ref=ret_ref.at[s],
            send_sem=a_sem.at[s],
            recv_sem=ra_sem.at[s],
            device_id=(z, s),
            device_id_type=MESH,
        )

    def place(t):
        return lax.rem(e + lax.rem(t, ne) + 1, ne)

    def risen(t):
        rise(b_ref, nd - 1 - t // ne, place(t)).wait_send()

    def fallen(t):
        fall(b_ref, t // ne, place(t)).wait_send()

    def weights(left, right, out, k):
        tiles = left.shape[1] // 128
        every = ne // tiles

        @pl.when(lax.rem(k, every) == 0)
        def _():
            cols = pl.ds(pl.multiple_of(k // every * 128, 128), 128)
            out[cols, :] = lax.dot_general(
                left[:, cols],
                right[...],
                (((0,), (0,)), ((), ())),
                preferred_element_type=jnp.float32,
            )

    def add(held, other, o, s):
        total = held[o, s].astype(jnp.float32) + other[o, s].astype(jnp.float32)
        held[o, s] = total.astype(held.dtype)

    upper = (z >= nd // 2).astype(jnp.int32)

    def travel(step):
        t_up = step - lag * upper
        t_dn = step - lag * (1 - upper)

        @pl.when((t_up >= 0) & (t_up < (nd - 1 - z) * ne))
        def _():
            o = nd - 1 - t_up // ne
            s = place(t_up)

            @pl.when(t_up >= window)
            def _():
                risen(t_up - window)

            @pl.when(z == 0)
            def _():
                rise(b_ref, o, s).start()

            @pl.when(z > 0)
            def _():
                rise(from_dn, o, s).wait_recv()
                add(from_dn, b_ref, o, s)
                rise(from_dn, o, s).start()

        @pl.when((t_dn >= 0) & (t_dn < z * ne))
        def _():
            o = t_dn // ne
            s = place(t_dn)

            @pl.when(t_dn >= window)
            def _():
                fallen(t_dn - window)

            @pl.when(z == nd - 1)
            def _():
                fall(b_ref, o, s).start()

            @pl.when(z < nd - 1)
            def _():
                fall(from_up, o, s).wait_recv()
                add(from_up, b_ref, o, s)
                fall(from_up, o, s).start()

    for j in range(nd - 1):
        if j <= nd - 1 - j:
            produce(nd - 1 - j)
        if j < nd - 1 - j:
            produce(j)

        @pl.loop(0, ne)
        def _(k):
            travel(j * ne + k)
            if j == min(nd // 2, nd - 2):
                weights(x_ref, dpre_ref, gup_ref, k)
                weights(a_ref, d_ref, gdn_ref, k)

    @pl.loop((nd - 1) * ne, (nd - 1) * ne + lag)
    def _(step):
        travel(step)

    @pl.loop(0, ne)
    def _(k):
        s = lax.rem(e + k + 1, ne)

        @pl.when(z > 0)
        def _():
            rise(from_dn, z, s).wait_recv()
            add(b_ref, from_dn, z, s)

        @pl.when(z < nd - 1)
        def _():
            fall(from_up, z, s).wait_recv()
            add(b_ref, from_up, z, s)

        @pl.when(s != e)
        def _():
            cross(s).start()

        @pl.when(s == e)
        def _():
            ret_ref[e] = b_ref[z, e]

    @pl.loop(1, ne)
    def _(k):
        back(lax.rem(e + ne - k, ne)).wait_recv()

    @pl.loop(1, ne)
    def _(k):
        cross(lax.rem(e + k, ne)).wait_send()

    @pl.loop(0, window)
    def _(i):
        @pl.when(z < nd - 1)
        def _():
            risen((nd - 1 - z) * ne - window + i)

        @pl.when(z > 0)
        def _():
            fallen(z * ne - window + i)

    router_arrive()
    router_drain()

def bring_back(xe, slope, weights, q, h, c, a, d, router_part, nd, ne):
    total, width = xe.shape
    hidden = slope.shape[1]
    n = nd * ne
    height = total // n
    dtype = jnp.bfloat16
    dma = pltpu.SemaphoreType.DMA
    return pl.pallas_call(
        functools.partial(bring_kernel, nd, ne),
        out_shape=(
            jax.ShapeDtypeStruct((ne, height, width), dtype),
            jax.ShapeDtypeStruct((width, hidden), jnp.float32),
            jax.ShapeDtypeStruct((hidden, width), jnp.float32),
            jax.ShapeDtypeStruct((n,) + router_part.shape, jnp.float32),
        ),
        in_specs=[vmem()] * 9,
        out_specs=(vmem(),) * 4,
        scratch_shapes=[
            pltpu.VMEM((nd, ne, height, width), dtype),
            pltpu.VMEM((total, hidden), dtype),
            pltpu.VMEM((nd, ne, height, width), dtype),
            pltpu.VMEM((nd, ne, height, width), dtype),
            dma((nd, ne)),
            dma((nd, ne)),
            dma((nd, ne)),
            dma((nd, ne)),
            dma((ne,)),
            dma((ne,)),
            dma((n,)),
            dma((n,)),
        ],
        compiler_params=pltpu.CompilerParams(has_side_effects=True),
        name="bring_back",
    )(xe, slope, weights, q, h, c, a, d, router_part)


def spread(nd, ne, me, src, dst, send_sem, recv_sem):
    n = nd * ne

    def copy(t, sender):
        return pltpu.make_async_remote_copy(
            src_ref=src(t),
            dst_ref=dst.at[sender],
            send_sem=send_sem.at[t],
            recv_sem=recv_sem.at[sender],
            device_id=(t // ne, lax.rem(t, ne)),
            device_id_type=MESH,
        )

    @pl.loop(1, n)
    def _(k):
        copy(lax.rem(me + k, n), me).start()

    def arrive():
        @pl.loop(1, n)
        def _(k):
            t = lax.rem(me + n - k, n)
            copy(t, t).wait_recv()

    def drain():
        @pl.loop(1, n)
        def _(k):
            copy(lax.rem(me + k, n), me).wait_send()

    return arrive, drain


def pairs_kernel(nd, ne, m_ref, x_ref, out_ref, held, own, s1, r1, s2, r2):
    me = lax.axis_index("dp") * ne + lax.axis_index("expert")
    held[me] = m_ref[me]
    arrive, drain_first = spread(nd, ne, me, lambda t: m_ref.at[t], held, s1, r1)
    arrive()
    total = jnp.sum(held[...], axis=0) + x_ref[...]
    own[...] = total
    out_ref[me] = total
    arrive, drain_second = spread(nd, ne, me, lambda t: own, out_ref, s2, r2)
    arrive()
    drain_first()
    drain_second()


def pair_sums(m, x, nd, ne):
    n = nd * ne
    dma = pltpu.SemaphoreType.DMA
    return pl.pallas_call(
        functools.partial(pairs_kernel, nd, ne),
        out_shape=jax.ShapeDtypeStruct(m.shape, m.dtype),
        in_specs=[vmem(), vmem()],
        out_specs=vmem(),
        scratch_shapes=[
            pltpu.VMEM(m.shape, m.dtype),
            pltpu.VMEM(x.shape, x.dtype),
            dma((n,)),
            dma((n,)),
            dma((n,)),
            dma((n,)),
        ],
        compiler_params=pltpu.CompilerParams(has_side_effects=True),
        name="pair_sums",
    )(m, x)


def everyone_kernel(nd, ne, x_ref, out_ref, held, own, planes, s1, r1, s2, r2):
    z = lax.axis_index("dp")
    e = lax.axis_index("expert")

    def across(t, sender):
        return pltpu.make_async_remote_copy(
            src_ref=x_ref,
            dst_ref=held.at[sender],
            send_sem=s1.at[t],
            recv_sem=r1.at[sender],
            device_id=(z, t),
            device_id_type=MESH,
        )

    def along(t, sender):
        return pltpu.make_async_remote_copy(
            src_ref=own,
            dst_ref=planes.at[sender],
            send_sem=s2.at[t],
            recv_sem=r2.at[sender],
            device_id=(t, e),
            device_id_type=MESH,
        )

    def exchange(count, here, copy):
        @pl.loop(1, count)
        def _(k):
            copy(lax.rem(here + k, count), here).start()

        @pl.loop(1, count)
        def _(k):
            t = lax.rem(here + count - k, count)
            copy(t, t).wait_recv()

    def drain(count, here, copy):
        @pl.loop(1, count)
        def _(k):
            copy(lax.rem(here + k, count), here).wait_send()

    held[e] = x_ref[...]
    exchange(ne, e, across)
    total = jnp.sum(held[...], axis=0)
    own[...] = total
    planes[z] = total
    exchange(nd, z, along)
    out_ref[...] = jnp.sum(planes[...], axis=0)
    drain(ne, e, across)
    drain(nd, z, along)


def everyone(x, nd, ne):
    dma = pltpu.SemaphoreType.DMA
    return pl.pallas_call(
        functools.partial(everyone_kernel, nd, ne),
        out_shape=jax.ShapeDtypeStruct(x.shape, x.dtype),
        in_specs=[vmem()],
        out_specs=vmem(),
        scratch_shapes=[
            pltpu.VMEM((ne,) + x.shape, x.dtype),
            pltpu.VMEM(x.shape, x.dtype),
            pltpu.VMEM((nd,) + x.shape, x.dtype),
            dma((ne,)),
            dma((ne,)),
            dma((nd,)),
            dma((nd,)),
        ],
        compiler_params=pltpu.CompilerParams(has_side_effects=True),
        name="everyone",
    )(x)


def body(
    tokens,
    expert_ids,
    caption_lengths,
    layer_norm_gain,
    router,
    w_up,
    w_down,
    logit_scale,
    logit_bias,
):
    nd = lax.axis_size("dp")
    ne = lax.axis_size("expert")
    n = nd * ne
    assert tokens.shape[0] == 1 and w_up.shape[0] == 1
    rows = SEQ
    experts = router.shape[1]
    slots = rows * 4 // (3 * experts) + 1
    height = -(-(slots + 1) // 8) * 8
    total = n * height
    expert = lax.axis_index("expert")
    me = lax.axis_index("dp") * ne + expert
    wu, wd = w_up[0], w_down[0]

    x = tokens.reshape(rows, D).astype(jnp.float32)
    mean = jnp.mean(x, axis=1, keepdims=True)
    var = jnp.mean((x - mean) ** 2, axis=1, keepdims=True)
    rstd = 1.0 / jnp.sqrt(var + eps)
    xhat = (x - mean) * rstd
    xn = (xhat * layer_norm_gain).astype(jnp.bfloat16)

    ids = expert_ids.reshape(rows)
    onehot = ids[:, None] == jnp.arange(experts, dtype=jnp.int32)[None, :]
    earlier = jnp.arange(rows)[:, None] > jnp.arange(rows)[None, :]
    before = dot(earlier.astype(jnp.bfloat16), onehot.astype(jnp.bfloat16), ((1,), (0,)))
    slot = jnp.sum(jnp.where(onehot, before, 0.0), axis=1).astype(jnp.int32)
    dest = ids * height + slot
    place = (jnp.arange(experts * height, dtype=jnp.int32)[:, None] == dest[None, :]).astype(
        jnp.bfloat16
    )
    length = caption_lengths.astype(jnp.float32)
    row = jnp.arange(rows, dtype=jnp.int32)
    mark = jnp.where(row < PATCH, -1.0, jnp.where(row - PATCH < caption_lengths[0], length[0], 0.0))
    marks = jnp.sum(place.astype(jnp.float32) * mark[None, :], axis=1).reshape(experts, 1, height)
    marks = jnp.pad(marks, ((0, 0), (0, 0), (0, D - height)))
    packed = dot(place, xn, ((1,), (0,))).reshape(experts, height, D)
    is_mark = (jnp.arange(height) == slots)[None, :, None]
    packed = jnp.where(is_mark, marks, packed).astype(jnp.bfloat16)

    got, act, slope = dispatch(packed, wu, nd, ne)
    act, slope = act.reshape(total, -1), slope.reshape(total, -1)
    xe = got.reshape(total, D)

    marks = got.reshape(n, height, D)[:, slots, :height].astype(jnp.float32)
    marks = jnp.where(jnp.arange(height)[None, :] < slots, marks, 0.0).reshape(total)
    is_img, is_txt = marks < 0.0, marks > 0.0
    weight = jnp.where(is_img, 1.0 / PATCH, jnp.where(is_txt, 1.0 / jnp.maximum(marks, 1.0), 0.0))
    column = lax.dynamic_slice_in_dim(router, expert, 1, axis=1)
    columns = jnp.concatenate(split3(column), axis=1)
    gate = jax.nn.sigmoid(jnp.sum(dot(xe, columns, ((1,), (0,))), axis=1))
    coef_row = weight * gate
    kind = jnp.arange(2 * n, dtype=jnp.int32)[:, None]
    pair_of = jnp.arange(total, dtype=jnp.int32)[None, :] // height
    member = (kind // 2 == pair_of) & ((kind % 2 == 0) == is_img[None, :])
    q_high, q_low = split(jnp.where(member, coef_row[None, :], 0.0))
    both = dot(jnp.concatenate([q_high, q_low], axis=0), act, ((1,), (0,)))
    a = both[: 2 * n] + both[2 * n :]
    a_high, a_low = split(a)
    both = dot(jnp.concatenate([a_high, a_low], axis=0), wd, ((1,), (0,)))
    moe_sums = both[: 2 * n] + both[2 * n :]

    img_x = jnp.sum(x[:PATCH], axis=0) / PATCH
    mask = (jnp.arange(CAPLEN, dtype=jnp.int32) < caption_lengths[0]).astype(jnp.float32)
    txt_x = jnp.sum(x[PATCH:] * mask[:, None], axis=0) / length[0]
    own_x = jnp.concatenate([img_x, txt_x]).reshape(8, 2 * D // 8)
    sums = pair_sums(moe_sums.reshape(n, 8, 2 * D // 8), own_x, nd, ne).reshape(n, 2, D)
    img, txt = sums[:, 0], sums[:, 1]

    ru = jnp.sqrt(jnp.mean(img * img, axis=1, keepdims=True) + eps)
    rv = jnp.sqrt(jnp.mean(txt * txt, axis=1, keepdims=True) + eps)
    u, v = img / ru, txt / rv
    scale = logit_scale[0]
    logits = (
        scale * lax.dot_general(u, v, (((1,), (1,)), ((), ())), precision=HIGHEST) / D
        + logit_bias[0]
    )
    sign = 2.0 * jnp.eye(n, dtype=jnp.float32) - 1.0
    loss = -jnp.sum(jax.nn.log_sigmoid(sign * logits)) / n
    coef = -(loss_scale / n) * sign * jax.nn.sigmoid(-sign * logits)
    du = scale / D * jnp.dot(coef, v, precision=HIGHEST)
    dv = scale / D * lax.dot_general(coef, u, (((0,), (0,)), ((), ())), precision=HIGHEST)
    dimg = (du - u * jnp.mean(du * u, axis=1, keepdims=True)) / ru
    dtxt = (dv - v * jnp.mean(dv * v, axis=1, keepdims=True)) / rv
    dvec = jnp.stack([dimg, dtxt], axis=1).reshape(2 * n, D)
    d_high, d_low = split(dvec)

    both = dot(jnp.concatenate([d_high, d_low], axis=0), wd, ((1,), (1,)))
    dhid = both[: 2 * n] + both[2 * n :]
    h_high, h_low = split(dhid)
    both = dot(act, jnp.concatenate([h_high, h_low], axis=0), ((1,), (1,)))
    products = jnp.where(member.T, both[:, : 2 * n] + both[:, 2 * n :], 0.0)
    dgl = jnp.sum(products, axis=1) * weight * gate * (1.0 - gate)
    router_part = jnp.sum(dot(jnp.stack(split3(dgl)), xe, ((1,), (0,))), axis=0)
    local = jnp.arange(2 * ne, dtype=jnp.int32)[None, :]
    pair_in_plane = lax.rem(jnp.arange(total, dtype=jnp.int32)[:, None] // height, ne)
    own = (local // 2 == pair_in_plane) & ((local % 2 == 0) == is_img[:, None])
    qt_high, qt_low = split(jnp.where(own, coef_row[:, None], 0.0))
    h_high, h_low = h_high.reshape(nd, 2 * ne, -1), h_low.reshape(nd, 2 * ne, -1)
    g_high, g_low = split(dgl[:, None])
    c_high, c_low = split(column.T)
    returned, grad_up, grad_down, router_all = bring_back(
        xe,
        slope,
        wu,
        jnp.concatenate([qt_high, qt_high, qt_low, g_high, g_high, g_low], axis=1),
        jnp.pad(jnp.concatenate([h_high, h_low, h_high], axis=1), ((0, 0), (0, 3), (0, 0))),
        jnp.pad(jnp.concatenate([c_high, c_low, c_high], axis=0), ((6 * ne, 0), (0, 0))),
        jnp.concatenate([a_high, a_high, a_low], axis=0),
        jnp.concatenate([d_high, d_low, d_high], axis=0),
        router_part.reshape(8, D // 8),
        nd,
        ne,
    )
    grad_up, grad_down = grad_up[None], grad_down[None]

    dxn = dot(place, returned.reshape(experts * height, D), ((0,), (0,)))
    gain_part = jnp.sum(dxn * xhat, axis=0)
    g = dxn * layer_norm_gain
    normed = (
        g - jnp.mean(g, axis=1, keepdims=True) - xhat * jnp.mean(g * xhat, axis=1, keepdims=True)
    ) * rstd
    mine = lax.dynamic_slice_in_dim(dvec, 2 * me, 2, axis=0)
    dy = jnp.where(
        (row < PATCH)[:, None],
        mine[0:1] / PATCH,
        jnp.where(mark > 0.0, 1.0 / length[0], 0.0)[:, None] * mine[1:2],
    )
    grad_tokens = (dy + normed).astype(jnp.bfloat16).reshape(1, SEQ, D)
    gain_grad = everyone(gain_part.reshape(8, D // 8), nd, ne).reshape(D)
    grad_router = jnp.sum(router_all.reshape(nd, ne, D), axis=0).T
    return (loss.reshape(1), grad_tokens, grad_up, grad_down, grad_router, gain_grad)


def solution(mesh):
    return jax.shard_map(
        body,
        mesh=mesh,
        in_specs=(
            P(("dp", "expert"), None, None),
            P(("dp", "expert"), None, None),
            P(("dp", "expert")),
            P(),
            P(),
            P("expert", None, "dp"),
            P("expert", "dp", None),
            P(),
            P(),
        ),
        out_specs=(
            P(),
            P(("dp", "expert"), None, None),
            P("expert", None, "dp"),
            P("expert", "dp", None),
            P(),
            P(),
        ),
        check_vma=False,
    )
```
